128 devices in a mesh: along: 8 (over z, core), across: 4 (over y), chan: 4 (over x).
Axes of the slice: x: 4, y: 4, z: 4, core: 2. Of those that a mesh axis runs over, the one named last changes fastest.
Arguments:
- jacobian: float32 [32, 32, 512, 384], P('along', 'across', 'chan'), may hold values from -0.3125 to 0.3125
- departures: float32 [32, 32, 512], P('along', 'across', 'chan'), may hold values from -6 to 6
- inv_variance: float32 [512], P('chan'), may hold values from 0.3 to 3
- channel_use: int32 [512], P('chan'), may hold values 0 or 1
- clear_flags: int32 [32, 32], P('along', 'across'), may hold values 0 or 1
- coefficients: float32 [25, 384], replicated, may hold values from -1.25 to 1.25
Outputs:
- control: float32 [32, 32, 384], P('along', 'across')
- increment: float32 [32, 32, 384], P('along', 'across')
- residual: float32 [32, 32, 384], P('along', 'across')
The draws below stay inside these ranges and needn't reach their ends.
All inputs are finite; a program needn't handle non-finite values. No bound on the sum of `channel_use` or of `clear_flags` on one device may be relied on, other than what follows from the above.
Results may differ from the reference program's by a relative error of at most 0.0003.
Values sent between devices are 32-bit elements; how exact they have to be, the bound alone decides.
No kernel may reach another device: no remote copies, remote signals or barrier semaphores. Data moves between devices by JAX's collectives and lax.ppermute only.
A program may use at most 64 MiB of HBM per device.

```python
import math
import jax
import jax.numpy as jnp
from jax import lax

CH = 512
ITERS = 10
S = 384
NX = 32
NY = 32


def set_ends(drawn, rng, smallest, top_value):
    extent = drawn.shape
    place = [jax.random.randint(jax.random.fold_in(rng, axis), (), 0, extent[axis]) for axis in range(len(extent))]
    drawn = drawn.at[tuple(place)].set(smallest)
    longest = extent.index(max(extent))
    place[longest] = (place[longest] + 1) % extent[longest]
    return drawn.at[tuple(place)].set(top_value)


def block_levels(stream_key, shape, pieces, least, top_value):
    gain, own = 1.0, jax.random.fold_in(stream_key, 6)
    for dim, shards_of in pieces:
        steps = jnp.exp(jax.random.uniform(jax.random.fold_in(own, dim), (shards_of,), jnp.float32, least / len(pieces), top_value / len(pieces)))
        gain = gain * jnp.repeat(steps, shape[dim] // shards_of).reshape([-1 if axis == dim else 1 for axis in range(len(shape))])
    return gain


def noise(stream_key, extent, width, reach, shards=(), kind=jnp.bfloat16):
    values = jax.random.normal(stream_key, extent, jnp.float32) * width
    if len(shards) > 0:
        values = block_levels(stream_key, extent, shards, -0.22, 0.18) * values
    return jnp.clip(values, min=-reach, max=reach).astype(kind)


def setup_inputs(seed: int = 0) -> dict:
    key_of = jax.random.split(jax.random.key(seed), 7)
    jacobian = noise(key_of[0], (NX, NY, CH, S), S ** -0.5, 0.3125, ((0, 8), (1, 4), (2, 4)), jnp.float32)
    departures = noise(key_of[1], (NX, NY, CH), 1.0, 6.0, ((0, 8), (1, 4), (2, 4)), jnp.float32)
    inv_variance = jnp.clip(jnp.exp(math.log(3.0) - 2.3025851 * jax.random.uniform(key_of[2], (CH,), jnp.float32) ** block_levels(key_of[2], (CH,), ((0, 4),), -0.2, 0.2)), 0.3, 3.0)
    channel_use = set_ends((jax.random.randint(key_of[3], (CH,), 0, 4) < 3).astype(jnp.int32), jax.random.fold_in(key_of[3], 1), 0, 1)
    clear_flags = set_ends((jax.random.randint(key_of[4], (NX, NY), 0, 4) < 3).astype(jnp.int32), jax.random.fold_in(key_of[4], 1), 0, 1)
    coefficients = noise(key_of[5], (25, S), 25 ** -0.5, 1.25, (), jnp.float32)
    return {"jacobian": jacobian, "departures": departures, "inv_variance": inv_variance, "channel_use": channel_use, "clear_flags": clear_flags, "coefficients": coefficients}


def spread(field, coefficients):
    rows_here, cols_here = field.shape[0], field.shape[1]
    padded = jnp.pad(field, ((2, 2), (2, 2), (0, 0)))
    result = jnp.zeros(field.shape, jnp.float32)
    for row_shift in range(5):
        for col_shift in range(5):
            result = result + coefficients[row_shift * 5 + col_shift] * padded[row_shift:row_shift + rows_here, col_shift:col_shift + cols_here]
    return result


def spread_back(field, coefficients):
    rows_here, cols_here = field.shape[0], field.shape[1]
    padded = jnp.pad(field, ((2, 2), (2, 2), (0, 0)))
    result = jnp.zeros(field.shape, jnp.float32)
    for row_shift in range(5):
        for col_shift in range(5):
            result = result + coefficients[row_shift * 5 + col_shift] * padded[4 - row_shift:4 - row_shift + rows_here, 4 - col_shift:4 - col_shift + cols_here]
    return result


def reference(jacobian, departures, inv_variance, channel_use, clear_flags, coefficients):
    weight = inv_variance[None, None, :] * channel_use.astype(jnp.float32)[None, None, :] * clear_flags.astype(jnp.float32)[:, :, None]

    def forward(field):
        return jnp.einsum('xycs,xys->xyc', jacobian, field, precision=lax.Precision.HIGHEST)

    def adjoint(weighted):
        return jnp.einsum('xycs,xyc->xys', jacobian, weighted, precision=lax.Precision.HIGHEST)

    def hessian(direction):
        return direction + spread_back(adjoint(weight * forward(spread(direction, coefficients))), coefficients)

    rhs = spread_back(adjoint(weight * departures), coefficients)
    control = jnp.zeros_like(rhs)
    residual = rhs
    direction = rhs
    norm_now = jnp.sum(residual * residual)
    for step_index in range(ITERS):
        image = hessian(direction)
        alpha = norm_now / jnp.sum(direction * image)
        control = control + alpha * direction
        residual = residual - alpha * image
        fresh_norm = jnp.sum(residual * residual)
        direction = residual + (fresh_norm / norm_now) * direction
        norm_now = fresh_norm
    return control, spread(control, coefficients), residual
```

```python
import jax
import jax.numpy as jnp
from jax import lax
from jax.experimental import pallas as pl
from jax.experimental.pallas import tpu as pltpu
from jax.sharding import PartitionSpec as P

BLOCKS = (2, 2, 2, 2, 2)
S = 384
F32 = jnp.float32
VEC = (4, 8, S)


def call(kernel, out_shapes, scratch=()):
    vmem = pl.BlockSpec(memory_space=pltpu.VMEM)

    def run(*args):
        return pl.pallas_call(
            kernel,
            out_shape=[jax.ShapeDtypeStruct(s, F32) for s in out_shapes],
            in_specs=[vmem] * len(args),
            out_specs=[vmem] * len(out_shapes),
            scratch_shapes=[pltpu.VMEM(s, F32) for s in scratch],
            compiler_params=pltpu.CompilerParams(vmem_limit_bytes=16 * 1024 * 1024),
        )(*args)

    return run


def project(jac, field, wcol, flag, out):
    def row(i, carry):
        x8 = field[i]
        sums = []
        for j in range(8):
            g = jac[i * 8 + j]
            y = jnp.sum(g * x8[j : j + 1, :], axis=1, keepdims=True)
            t = y * wcol[...]
            g3 = jac[i * 8 + j]
            sums.append(
                jnp.concatenate(
                    [
                        jnp.sum(g3[:, 128 * n : 128 * (n + 1)] * t, axis=0, keepdims=True)
                        for n in range(3)
                    ],
                    axis=1,
                )
            )
        out[i] = jnp.concatenate(sums, axis=0) * flag[i]
        return carry

    lax.fori_loop(0, 4, row, 0)


def first_kernel(jac, dep, wcol, flag, out):
    lane = lax.broadcasted_iota(jnp.int32, (128, 128), 1)
    sub = lax.broadcasted_iota(jnp.int32, (128, 128), 0)

    def row(i, carry):
        d8 = dep[i]
        sums = []
        for j in range(8):
            d = jnp.where(lane == sub, jnp.broadcast_to(d8[j : j + 1, :], (128, 128)), 0.0)
            t = jnp.sum(d, axis=1, keepdims=True) * wcol[...]
            g3 = jac[i * 8 + j]
            sums.append(
                jnp.concatenate(
                    [
                        jnp.sum(g3[:, 128 * n : 128 * (n + 1)] * t, axis=0, keepdims=True)
                        for n in range(3)
                    ],
                    axis=1,
                )
            )
        out[i] = jnp.concatenate(sums, axis=0) * flag[i]
        return carry

    lax.fori_loop(0, 4, row, 0)


def edges(total, to_right, to_left):
    for h in range(2):
        to_right[h] = jnp.concatenate([total[2 * h][4:], total[2 * h + 1][4:]], axis=0)
        to_left[h] = jnp.concatenate([total[2 * h][:4], total[2 * h + 1][:4]], axis=0)


def sum_kernel(own, near, far, other, total, to_right, to_left):
    total[...] = (own[...] + far[...]) + (near[...] + other[...])
    edges(total, to_right, to_left)


def fold(v):
    s = (v[0] + v[1]) + (v[2] + v[3])
    return (s[:, :128] + s[:, 128:256]) + s[:, 256:]


def sum_dot_kernel(own, near, far, other, uq, grams, total, to_right, to_left, scal):
    total[...] = (own[...] + far[...]) + (near[...] + other[...])
    edges(total, to_right, to_left)
    n = grams.shape[0]
    scal[: n - 1] = grams[: n - 1]
    scal[n - 1] = grams[n - 1] + fold(uq[...] * total[...])


def join_kernel(total, from_left, from_right, ctl, ext):
    keep = ctl[3][:, :1]
    for i in range(4):
        ext[i] = total[i]
        h, k = i // 2, 4 * (i % 2)
        side = jnp.concatenate([from_right[h][k : k + 4], from_left[h][k : k + 4]], axis=0)
        ext[4 + i] = jnp.where(keep > 0.5, side, 0.0)


def shifted(mid, side, d):
    if d == 0:
        return mid, side
    if d > 0:
        return (
            jnp.concatenate([mid[d:], side[:d]], axis=0),
            jnp.concatenate([side[d:], mid[:d]], axis=0),
        )
    d = -d
    return (
        jnp.concatenate([side[8 - d :], mid[: 8 - d]], axis=0),
        jnp.concatenate([mid[8 - d :], side[: 8 - d]], axis=0),
    )


def stencil(own, first, second, ctl, coef, wide, back, kw, kkw):
    odd, up_ok, down_ok = ctl[0][:, :1] > 0.5, ctl[1][:, :1] > 0.5, ctl[2][:, :1] > 0.5
    for i in range(4):
        for part in range(2):
            a, b = first[4 * part + i], second[4 * part + i]
            wide[i, part] = jnp.where(up_ok, jnp.where(odd, a, b), 0.0)
            wide[4 + i, part] = own[4 * part + i]
            wide[8 + i, part] = jnp.where(down_ok, jnp.where(odd, b, a), 0.0)
    side_ok = ctl[3][:, :1] > 0.5

    def back_row(i, carry):
        mid_sum = side_sum = 0.0
        for b in range(5):
            m = s = 0.0
            for a in range(5):
                c = coef[5 * a + b]
                m = m + c * wide[i + 4 - a, 0]
                s = s + c * wide[i + 4 - a, 1]
            m, s = shifted(m, s, 2 - b)
            mid_sum, side_sum = mid_sum + m, side_sum + s
        back[i, 0] = mid_sum
        back[i, 1] = jnp.where(side_ok, side_sum, 0.0)
        return carry

    lax.fori_loop(0, 8, back_row, 0)
    for i in range(2):
        for part in range(2):
            back[i, part] = jnp.where(up_ok, back[i, part], 0.0)
            back[6 + i, part] = jnp.where(down_ok, back[6 + i, part], 0.0)

    for i in range(4):
        kw[i] = back[i + 2, 0]

    def row(i, carry):
        total = 0.0
        for b in range(5):
            m = s = 0.0
            for a in range(5):
                c = coef[5 * a + b]
                m = m + c * back[i + a, 0]
                s = s + c * back[i + a, 1]
            total = total + shifted(m, s, b - 2)[0]
        kkw[i] = total
        return carry

    if kkw is not None:
        lax.fori_loop(0, 4, row, 0)


WIDE, BACK = (12, 2, 8, S), (8, 2, 8, S)


def start_kernel(ext, first, second, ctl, coef, jac, wcol, flag, u0, uq0, share, wide, back):
    stencil(ext, first, second, ctl, coef, wide, back, u0, uq0)
    project(jac, uq0, wcol, flag, share)


def inner_kernel(
    ext, first, second, ctl, coef, jac, wcol, flag, u0, uq0, ps, hps, steer,
    hu0, huq0, u1, uq1, grams, share, wide, back, kw, kkw,
):
    stencil(ext, first, second, ctl, coef, wide, back, kw, kkw)
    a = steer[0, :1, :1]
    hu0[...] = u0[...] + kw[...]
    huq0[...] = uq0[...] + kkw[...]
    u1[...] = hu0[...] - a * u0[...]
    uq1[...] = huq0[...] - a * uq0[...]
    v0, v1 = u0[...], u1[...]
    rows = [v0 * v0, v0 * v1, v0 * hu0[...], v1 * hu0[...]]
    for n in range(hps.shape[0]):
        rows += [hps[n] * v0, hps[n] * v1, ps[n] * v0]
    rows += [v1 * v1]
    for n, r in enumerate(rows):
        grams[n] = fold(r)
    project(jac, uq1, wcol, flag, share)


def solve(scal, known, count):
    total = [jnp.sum(scal[n], axis=(0, 1), keepdims=True) for n in range(scal.shape[0])]
    t0, t1, m00, m01 = total[:4]
    m11 = total[-1]
    cross = [total[4 + 3 * n : 7 + 3 * n] for n in range(count)]
    g0 = []
    d = m00
    y0, y1 = t0, t1
    off = m01
    last = m11
    g1 = []
    fixes = []
    for n in range(count):
        k = known[n][:1, :1]
        f0, f1 = cross[n][0] / k, cross[n][1] / k
        y0 = y0 - f0 * cross[n][2]
        y1 = y1 - f1 * cross[n][2]
        fixes.append(cross[n][2] / k)
        d = d - f0 * cross[n][0]
        off = off - f0 * cross[n][1]
        last = last - f1 * cross[n][1]
        g0.append(f0)
        g1.append(f1)
    e = off / d
    last = last - e * off
    alpha0 = y0 / d
    alpha1 = (y1 - e * y0) / last
    steer = m00 / t0
    return g0, g1, e, d, last, alpha0, alpha1, fixes, steer


def block_kernel(count, final):
    def body(*refs):
        refs = list(refs)
        take = lambda n: [refs.pop(0) for _ in range(n)]
        ext, first, second, ctl, coef = take(5)
        if not final:
            jac, wcol, flag = take(3)
        scal, u0, uq0, hu0, huq0, u1, uq1, x, xq = take(9)
        if count:
            known, ps, hps, pqs, hpqs = take(5)
        if final:
            x_out, xq_out, r_out = take(3)
        else:
            (x_out, xq_out, r_out, q_out, ps_out, hps_out, pqs_out, hpqs_out, known_out, steer_out, share) = take(11)
        wide, back, kw, kkw = take(4)
        stencil(ext, first, second, ctl, coef, wide, back, kw, None if final else kkw)
        g0, g1, e, d0, d1, a0, a1, fixes, steer = solve(scal, known if count else None, count)

        def pair(old, v0, v1):
            p0, p1 = v0, v1
            for n in range(count):
                p0 = p0 - g0[n] * old[n]
                p1 = p1 - g1[n] * old[n]
            return p0, p1 - e * p0

        p0, p1 = pair(ps if count else None, u0[...], u1[...])
        h0, h1 = pair(hps if count else None, hu0[...], u1[...] + kw[...])

        def step(old, v0, v1):
            total = a0 * v0 + a1 * v1
            for n in range(count):
                total = total + fixes[n] * old[n]
            return total

        x_out[...] = x[...] + step(ps if count else None, p0, p1)
        r_out[...] = u0[...] - step(hps if count else None, h0, h1)
        q0, q1 = pair(pqs if count else None, uq0[...], uq1[...])
        xq_out[...] = xq[...] + step(pqs if count else None, q0, q1)
        if final:
            return
        hq0, hq1 = pair(hpqs if count else None, huq0[...], uq1[...] + kkw[...])
        q_out[...] = uq0[...] - step(hpqs if count else None, hq0, hq1)
        for n, v in enumerate((p0, p1)):
            ps_out[n] = v
        for n, v in enumerate((h0, h1)):
            hps_out[n] = v
        for n, v in enumerate((q0, q1)):
            pqs_out[n] = v
        for n, v in enumerate((hq0, hq1)):
            hpqs_out[n] = v
        for n, v in enumerate((d0, d1)):
            known_out[n] = jnp.broadcast_to(v, (8, 128))
        steer_out[0] = jnp.broadcast_to(steer, (8, 128))
        project(jac, q_out, wcol, flag, share)

    return body


def shift(x, axis, k):
    n = lax.axis_size(axis)
    return lax.ppermute(x, axis, [(i, (i + k) % n) for i in range(n)])


def swap(x, axis, bit):
    return lax.ppermute(x, axis, [(i, i ^ bit) for i in range(lax.axis_size(axis))])


def facing(x):
    n = lax.axis_size("along")
    return lax.ppermute(x, "along", [(i, (i - 1 if i % 2 == 0 else i + 1) % n) for i in range(n)])


def everywhere(scal):
    for axis in ("along", "across"):
        bit = 1
        while bit < lax.axis_size(axis):
            scal = scal + swap(scal, axis, bit)
            bit *= 2
    return scal


def on_device(jacobian, departures, inv_variance, channel_use, clear_flags, coefficients):
    jac = jacobian.reshape(32, 128, S)
    wcol = jnp.broadcast_to((inv_variance * channel_use.astype(F32))[:, None], (128, 128))
    flag = jnp.broadcast_to(clear_flags.astype(F32)[:, :, None], VEC)
    coef = jnp.broadcast_to(coefficients[:, None, :], (25, 8, S))
    a, c = lax.axis_index("along"), lax.axis_index("across")
    na, nc = lax.axis_size("along"), lax.axis_size("across")
    sub = lax.broadcasted_iota(jnp.int32, (8, 128), 0)
    ctl = jnp.stack(
        [
            jnp.full((8, 128), a % 2, jnp.int32),
            jnp.full((8, 128), a > 0, jnp.int32),
            jnp.full((8, 128), a < na - 1, jnp.int32),
            jnp.where(sub < 4, c < nc - 1, c > 0).astype(jnp.int32),
        ]
    ).astype(F32)
    consts = (ctl, coef)
    sweep = (jac, wcol, flag)
    half = (2, 8, S)
    zero = jnp.zeros(VEC, F32)

    def halo(total, to_right, to_left):
        (ext,) = call(join_kernel, [(8, 8, S)])(
            total, shift(to_right, "across", 1), shift(to_left, "across", -1), ctl
        )
        return ext, swap(ext, "along", 1), facing(ext)

    def gathered(share):
        return share, shift(share, "chan", 1), shift(share, "chan", 2), shift(share, "chan", -1)

    def exchange(share):
        return halo(*call(sum_kernel, [VEC, half, half])(*gathered(share)))

    def exchange_dot(share, uq, grams):
        total, to_right, to_left, scal = call(sum_dot_kernel, [VEC, half, half, grams.shape])(
            *gathered(share), uq, grams
        )
        return halo(total, to_right, to_left), everywhere(scal)

    (share,) = call(first_kernel, [VEC])(jac, departures, wcol, flag)
    u0, uq0, share = call(start_kernel, [VEC] * 3, [WIDE, BACK])(*exchange(share), *consts, *sweep)
    x = xq = zero
    steer = jnp.zeros((1, 8, 128), F32)
    old = ()
    hps = jnp.zeros((0, *VEC), F32)
    for number in range(5):
        count, final = (2 if number else 0), number == 4
        near = exchange(share)
        rows = 5 + 3 * count
        hargs = old[1:3]

        def inner(*refs, count=count):
            refs = list(refs)
            if not count:
                refs[10:10] = [jnp.zeros((0, *VEC), F32)] * 2
            inner_kernel(*refs)

        hu0, huq0, u1, uq1, grams, share = call(
            inner, [VEC] * 4 + [(rows, 8, 128), VEC], [WIDE, BACK, VEC, VEC]
        )(*near, *consts, *sweep, u0, uq0, *hargs, steer)
        near, scal = exchange_dot(share, uq1, grams)
        state = (scal, u0, uq0, hu0, huq0, u1, uq1, x, xq, *old)
        if final:
            return tuple(
                call(block_kernel(count, True), [VEC] * 3, [WIDE, BACK, VEC, VEC])(*near, *consts, *state)
            )
        stack = (2, *VEC)
        x, xq, u0, uq0, ps, hps, pqs, hpqs, known, steer, share = call(
            block_kernel(count, False),
            [VEC] * 4 + [stack] * 4 + [(2, 8, 128), (1, 8, 128), VEC],
            [WIDE, BACK, VEC, VEC],
        )(*near, *consts, *sweep, *state)
        old = (known, ps, hps, pqs, hpqs)


def solution(mesh):
    return jax.shard_map(
        on_device,
        mesh=mesh,
        in_specs=(
            P("along", "across", "chan", None),
            P("along", "across", "chan"),
            P("chan"),
            P("chan"),
            P("along", "across"),
            P(),
        ),
        out_specs=(
            P("along", "across", None),
            P("along", "across", None),
            P("along", "across", None),
        ),
        check_vma=False,
    )
```

```python
import jax
import jax.numpy as jnp
from jax import lax
from jax.experimental import pallas as pl
from jax.experimental.pallas import tpu as pltpu
from jax.sharding import PartitionSpec as P

BLOCKS = (2, 2, 3, 3)
ALONG, ACROSS, CHAN = "along", "across", "chan"
S = 384
F32 = jnp.float32
VEC = (4, 8, S)
WIDE, BACK = (12, 2, 8, S), (8, 2, 8, S)


def params():
    return pltpu.CompilerParams(vmem_limit_bytes=16 * 1024 * 1024)


class Refs(dict):
    __getattr__ = dict.__getitem__


def call(kernel, outs, ins, scratch=()):
    vmem = pl.BlockSpec(memory_space=pltpu.VMEM)
    args, in_tree = jax.tree.flatten(ins)
    shapes, out_tree = jax.tree.flatten(outs, is_leaf=lambda v: isinstance(v, tuple))
    n, m = len(args), len(args) + len(shapes)

    def body(*refs):
        kernel(Refs(in_tree.unflatten(refs[:n]) | out_tree.unflatten(refs[n:m])), *refs[m:])

    result = pl.pallas_call(
        body,
        out_shape=[jax.ShapeDtypeStruct(s, F32) for s in shapes],
        in_specs=[vmem] * len(args),
        out_specs=[vmem] * len(shapes),
        scratch_shapes=[pltpu.VMEM(s, F32) for s in scratch],
        compiler_params=params(),
    )(*args)
    return Refs(out_tree.unflatten(result))


def back_through(g_ref, at, t):
    return jnp.concatenate(
        [
            jnp.sum(g_ref[at, :, 128 * n : 128 * (n + 1)] * t, axis=0, keepdims=True)
            for n in range(3)
        ],
        axis=1,
    )


def project(jac, field, wcol, flag, out):
    def row(i, carry):
        x8 = field[i]
        sums = []
        for j in range(8):
            y = jnp.sum(jac[i * 8 + j] * x8[j : j + 1, :], axis=1, keepdims=True)
            sums.append(back_through(jac, i * 8 + j, y * wcol[...]))
        out[i] = jnp.concatenate(sums, axis=0) * flag[i]
        return carry

    lax.fori_loop(0, 4, row, 0)


def column(row, size):
    lane = lax.broadcasted_iota(jnp.int32, (size, size), 1)
    sub = lax.broadcasted_iota(jnp.int32, (size, size), 0)
    return jnp.sum(jnp.where(lane == sub, jnp.broadcast_to(row, (size, size)), 0.0), axis=1, keepdims=True)


def first_kernel(place, jac, dep, inv, use, clear, coef, wcol, flag, ctl, coefs, out):
    wcol[...] = jnp.broadcast_to(column(inv[...] * use[...].astype(F32), 128), (128, 128))
    for i in range(4):
        flag[i] = jnp.broadcast_to(column(clear[i : i + 1, :].astype(F32), 8), (8, S))
    for n in range(3):
        ctl[n] = jnp.broadcast_to(place[n], (8, 128)).astype(F32)
    low = lax.broadcasted_iota(jnp.int32, (8, 128), 0) < 4
    ctl[3] = jnp.where(low, jnp.broadcast_to(place[3], (8, 128)), jnp.broadcast_to(place[4], (8, 128))).astype(F32)
    for n in range(25):
        coefs[n] = jnp.broadcast_to(coef[n : n + 1, :], (8, S))
    def row(i, carry):
        d8 = dep[i]
        sums = []
        for j in range(8):
            t = column(d8[j : j + 1, :], 128) * wcol[...]
            sums.append(back_through(jac, i * 8 + j, t))
        out[i] = jnp.concatenate(sums, axis=0) * flag[i]
        return carry

    lax.fori_loop(0, 4, row, 0)


def fold(v):
    s = (v[0] + v[1]) + (v[2] + v[3])
    return (s[:, :128] + s[:, 128:256]) + s[:, 256:]


def put(ref, at, v):
    for n in range(3):
        ref[at + n] = v[:, 128 * n : 128 * (n + 1)]


def get(ref, at):
    return jnp.concatenate([ref[at + n] for n in range(3)], axis=1)


def sum_kernel(r):
    total = (r.own[...] + r.far[...]) + (r.near[...] + r.other[...])
    r.total[...] = total
    for h in range(2):
        put(r.to_right, 3 * h, jnp.concatenate([total[2 * h][4:], total[2 * h + 1][4:]], axis=0))
        put(r.to_left, 3 * h, jnp.concatenate([total[2 * h][:4], total[2 * h + 1][:4]], axis=0))
    if "grams" in r:
        count = r.grams.shape[0]
        for n in range(count):
            g = r.grams[n]
            if n == count - 1:
                g = g + fold(r.uq[...] * total)
            r.scal[n] = g
            r.to_right[6 + n] = g
            r.to_left[6 + n] = g


def join_kernel(r):
    keep = r.ctl[3][:, :1]
    left, right = r.from_left, r.from_right
    for i in range(4):
        put(r.ext, 3 * i, r.total[i])
        h, k = 3 * (i // 2), 4 * (i % 2)
        side = jnp.concatenate([get(right, h)[k : k + 4], get(left, h)[k : k + 4]], axis=0)
        put(r.ext, 12 + 3 * i, jnp.where(keep > 0.5, side, 0.0))
    if "scal" in r:
        for n in range(r.scal.shape[0]):
            s = (r.scal[n] + r.opposite[n]) + (left[6 + n] + right[6 + n])
            r.ext[24 + n] = s
            r.plane[n] = s


def part_kernel(r):
    for n in range(r.part.shape[0]):
        r.part[n] = (r.facing[24 + n] + r.beside[n]) + r.opposite[n]


def shifted(mid, side, d):
    if d == 0:
        return mid, side
    if d > 0:
        return (
            jnp.concatenate([mid[d:], side[:d]], axis=0),
            jnp.concatenate([side[d:], mid[:d]], axis=0),
        )
    d = -d
    return (
        jnp.concatenate([side[8 - d :], mid[: 8 - d]], axis=0),
        jnp.concatenate([mid[8 - d :], side[: 8 - d]], axis=0),
    )


def stencil(r, wide, back, kw, kkw):
    ctl, coef = r.ctl, r.coef
    odd, up_ok, down_ok = ctl[0][:, :1] > 0.5, ctl[1][:, :1] > 0.5, ctl[2][:, :1] > 0.5
    for i in range(4):
        for part in range(2):
            at = 12 * part + 3 * i
            a, b = get(r.first, at), get(r.second, at)
            wide[i, part] = jnp.where(up_ok, jnp.where(odd, a, b), 0.0)
            wide[4 + i, part] = get(r.ext, at)
            wide[8 + i, part] = jnp.where(down_ok, jnp.where(odd, b, a), 0.0)
    side_ok = ctl[3][:, :1] > 0.5

    def back_row(i, carry):
        mid_sum = side_sum = 0.0
        for b in range(5):
            m = s = 0.0
            for a in range(5):
                c = coef[5 * a + b]
                m = m + c * wide[i + 4 - a, 0]
                s = s + c * wide[i + 4 - a, 1]
            m, s = shifted(m, s, 2 - b)
            mid_sum, side_sum = mid_sum + m, side_sum + s
        back[i, 0] = mid_sum
        back[i, 1] = jnp.where(side_ok, side_sum, 0.0)
        return carry

    lax.fori_loop(0, 8, back_row, 0)
    for i in range(2):
        for part in range(2):
            back[i, part] = jnp.where(up_ok, back[i, part], 0.0)
            back[6 + i, part] = jnp.where(down_ok, back[6 + i, part], 0.0)
    for i in range(4):
        kw[i] = back[i + 2, 0]

    def row(i, carry):
        total = 0.0
        for b in range(5):
            m = s = 0.0
            for a in range(5):
                c = coef[5 * a + b]
                m = m + c * back[i + a, 0]
                s = s + c * back[i + a, 1]
            total = total + shifted(m, s, b - 2)[0]
        kkw[i] = total
        return carry

    if kkw is not None:
        lax.fori_loop(0, 4, row, 0)


def start_kernel(r, wide, back):
    stencil(r, wide, back, r.u0, r.uq0)
    project(r.jac, r.uq0, r.wcol, r.flag, r.share)


def gram_rows(s, count):
    rows = [("t", k) for k in range(s)]
    rows += [("m", i, j) for i in range(s) for j in range(i, s) if i < s - 1]
    rows += [("x", n, k) for n in range(count) for k in range(s)]
    rows += [("f", n) for n in range(count)] + [("uu",)]
    return rows


def inner_kernel(k, s, count):
    def body(r, wide, back, kw, kkw):
        stencil(r, wide, back, kw, kkw)
        if "steer" in r:
            a, b = r.steer[0][:1, :1], r.steer[1][:1, :1]
        for basis, image, vector, q in ((r.us, r.image, r.u, kw), (r.uqs, r.imageq, r.uq, kkw)):
            v = basis[k - 1][...] + q[...]
            image[...] = v
            if "steer" in r:
                v = v - a * basis[k - 1][...]
                if k > 1:
                    v = v - b * basis[k - 2][...]
            vector[...] = v
        project(r.jac, r.uq, r.wcol, r.flag, r.share)
        if k < s - 1:
            return
        us, hus = [*r.us, r.u], [*r.hus, r.image]
        tiles = []
        for row in gram_rows(s, count):
            if row[0] == "t":
                x, y = us[row[1]][...], us[0][...]
            elif row[0] == "m":
                x, y = hus[row[1]][...], us[row[2]][...]
            elif row[0] == "x":
                x, y = r.hps[row[1]], us[row[2]][...]
            elif row[0] == "f":
                x, y = r.ps[row[1]], us[0][...]
            else:
                x, y = us[1][...], us[1][...]
            tiles.append(jnp.sum(fold(x * y), axis=0, keepdims=True))
        while len(tiles) % 8:
            tiles.append(jnp.zeros((1, 128), F32))
        for n in range(len(tiles) // 8):
            r.grams[n] = jnp.concatenate(tiles[8 * n : 8 * n + 8], axis=0)
        last = us[s - 1][...]
        r.grams[len(tiles) // 8] = fold(last * last)

    return body


def solve(scal, known, s, count, first):
    rows = gram_rows(s, count)
    packed = [jnp.sum(tile, axis=1, keepdims=True) for tile in scal[:-1]]
    val = {row: packed[n // 8][n % 8 : n % 8 + 1, :] for n, row in enumerate(rows)}
    w = {(i, j): val["m", i, j] for i in range(s) for j in range(i, s) if i < s - 1}
    w[s - 1, s - 1] = jnp.sum(scal[-1], axis=(0, 1), keepdims=True)
    y = [val["t", k] for k in range(s)]
    a = val["m", 0, 0] / y[0]
    b = (val["uu",] - y[1] * y[1] / y[0]) / y[0]
    inverse = [1.0 / known[n][:1, :1] for n in range(count)]
    old = [[val["x", n, k] * inverse[n] for k in range(s)] for n in range(count)]
    for n in range(count):
        for i in range(s):
            y[i] = y[i] - old[n][i] * val["f", n]
            for j in range(i, s):
                w[i, j] = w[i, j] - old[n][i] * val["x", n, j]
    new = {}
    for k in range(s):
        for i in range(k + 1, s):
            new[i, k] = w[k, i] / w[k, k]
        for i in range(k + 1, s):
            y[i] = y[i] - new[i, k] * y[k]
            for j in range(i, s):
                w[i, j] = w[i, j] - new[i, k] * w[k, j]
    fixes = [val["f", n] * inverse[n] for n in range(count)]
    pivots = [w[k, k] for k in range(s)]
    steps = [y[k] / w[k, k] for k in range(s)]
    return old, new, pivots, steps, fixes, (a, b if first else 0.5 * b)


def block_kernel(s, count, keep, first, final):
    def body(r, wide, back, kw, kkw):
        stencil(r, wide, back, kw, None if final else kkw)
        at = 24
        scal = [
            (r.ext[at + n] + r.first[at + n]) + (r.part[n] + r.mate[n])
            for n in range(r.part.shape[0])
        ]
        known = [r.known[n] for n in range(count)]
        old, new, pivots, steps, fixes, steer = solve(scal, known, s, count, first)

        def directions(stack, vectors):
            made = []
            for k, v in enumerate(vectors):
                for n in range(count):
                    v = v - old[n][k] * r.stacks[stack][n]
                for j in range(k):
                    v = v - new[k, j] * made[j]
                made.append(v)
            if not final:
                kept = [r.stacks[stack][n] for n in range(count)] + made
                for n, v in enumerate(kept[-keep:]):
                    r.stacks_new[stack][n] = v
            moved = steps[0] * made[0]
            for k in range(1, s):
                moved = moved + steps[k] * made[k]
            for n in range(count):
                moved = moved + fixes[n] * r.stacks[stack][n]
            return moved

        us, uqs, hus, huqs = ([v[...] for v in vs] for vs in (r.us, r.uqs, r.hus, r.huqs))
        moved = directions(0, us)
        r.x_new[...] = moved if first else r.x[...] + moved
        moved = directions(1, uqs)
        r.xq_new[...] = moved if first else r.xq[...] + moved
        r.r_new[...] = us[0] - directions(2, hus + [us[s - 1] + kw[...]])
        if final:
            return
        r.q_new[...] = uqs[0] - directions(3, huqs + [uqs[s - 1] + kkw[...]])
        kept = known + [jnp.broadcast_to(v, (8, 128)) for v in pivots]
        for n, v in enumerate(kept[-keep:]):
            r.known_new[n] = v
        for n, v in enumerate(steer):
            r.steer_new[n] = jnp.broadcast_to(v, (8, 128))
        project(r.jac, r.q_new, r.wcol, r.flag, r.share)

    return body


def move(x, axis, target):
    return lax.ppermute(x, axis, [(i, target(i)) for i in range(lax.axis_size(axis))])


def shift(x, axis, k):
    n = lax.axis_size(axis)
    return move(x, axis, lambda i: (i + k) % n)


def on_device(jacobian, departures, inv_variance, channel_use, clear_flags, coefficients):
    along, across = lax.axis_size(ALONG), lax.axis_size(ACROSS)
    a, c = lax.axis_index(ALONG), lax.axis_index(ACROSS)
    place = jnp.stack([a % 2, a > 0, a < along - 1, c < across - 1, c > 0]).astype(jnp.int32)
    vmem = pl.BlockSpec(memory_space=pltpu.VMEM)
    shapes = ((128, 128), VEC, (4, 8, 128), (25, 8, S), VEC)
    jac = jacobian.reshape(32, 128, S)
    wcol, flag, ctl, coef, share = pl.pallas_call(
        first_kernel,
        out_shape=[jax.ShapeDtypeStruct(s, F32) for s in shapes],
        in_specs=[pl.BlockSpec(memory_space=pltpu.SMEM)] + [vmem] * 6,
        out_specs=[vmem] * 5,
        compiler_params=params(),
    )(
        place,
        jac,
        departures,
        inv_variance[None],
        channel_use[None],
        clear_flags,
        coefficients,
    )
    consts = dict(ctl=ctl, coef=coef)
    sweep = dict(jac=jac, wcol=wcol, flag=flag)

    def exchange(share, sums=None):
        ins = dict(
            own=share,
            near=shift(share, CHAN, 1),
            far=shift(share, CHAN, 2),
            other=shift(share, CHAN, -1),
        )
        g = sums["grams"].shape[0] if sums else 0
        tail = (g, 8, 128)
        edge = (6 + g, 8, 128)
        outs = dict(total=VEC, to_right=edge, to_left=edge)
        if sums:
            ins |= sums
            outs |= dict(scal=tail)
        summed = call(sum_kernel, outs, ins)
        ins = dict(
            total=summed.total,
            from_left=shift(summed.to_right, ACROSS, 1),
            from_right=shift(summed.to_left, ACROSS, -1),
            ctl=ctl,
        )
        outs = dict(ext=(24 + g, 8, 128))
        if sums:
            ins |= dict(scal=summed.scal, opposite=shift(summed.scal, ACROSS, 2))
            outs |= dict(plane=tail)
        joined = call(join_kernel, outs, ins)
        ext = joined.ext
        near = dict(
            ext=ext,
            first=move(ext, ALONG, lambda i: i ^ 1),
            second=move(ext, ALONG, lambda i: (i - 1 if i % 2 == 0 else i + 1) % along),
        )
        if sums:
            plane = joined.plane
            ins = dict(
                facing=near["second"],
                beside=move(plane, ALONG, lambda i: (i + 2 if i % 2 == 0 else i - 2) % along),
                opposite=shift(plane, ALONG, 4),
            )
            part = call(part_kernel, dict(part=tail), ins).part
            near |= dict(part=part, mate=move(part, ALONG, lambda i: i ^ 1))
        return near | consts

    work = [WIDE, BACK]
    more = [WIDE, BACK, VEC, VEC]
    made = call(start_kernel, dict(u0=VEC, uq0=VEC, share=VEC), exchange(share) | sweep, work)
    us, uqs, hus, huqs = [made.u0], [made.uq0], [], []
    share = made.share
    state = old = steer = {}
    count = 0
    for number, s in enumerate(BLOCKS):
        final = number == len(BLOCKS) - 1
        for k in range(1, s):
            outs = dict(image=VEC, imageq=VEC, u=VEC, uq=VEC, share=VEC)
            ins = exchange(share) | sweep | steer | dict(us=us, uqs=uqs)
            if k == s - 1:
                outs |= dict(grams=(-(-len(gram_rows(s, count)) // 8) + 1, 8, 128))
                ins |= dict(hus=hus)
                if count:
                    ins |= dict(ps=old["stacks"][0], hps=old["stacks"][2])
            made = call(inner_kernel(k, s, count), outs, ins, more)
            share = made.share
            us, uqs = us + [made.u], uqs + [made.uq]
            hus, huqs = hus + [made.image], huqs + [made.imageq]
        near = exchange(share, dict(grams=made.grams, uq=made.uq))
        keep = 0 if final else min(count + s, BLOCKS[number + 1])
        ins = near | state | old | dict(us=us, uqs=uqs, hus=hus, huqs=huqs)
        outs = dict(x_new=VEC, xq_new=VEC, r_new=VEC)
        if not final:
            ins |= sweep
            outs |= dict(q_new=VEC, share=VEC, known_new=(keep, 8, 128), steer_new=(2, 8, 128))
            outs |= dict(stacks_new=[(keep, *VEC)] * 4)
        made = call(block_kernel(s, count, keep, number == 0, final), outs, ins, more)
        if final:
            return made.x_new, made.xq_new, made.r_new
        count = keep
        state = dict(x=made.x_new, xq=made.xq_new)
        us, uqs, hus, huqs = [made.r_new], [made.q_new], [], []
        share = made.share
        steer = dict(steer=made.steer_new)
        old = dict(known=made.known_new, stacks=made.stacks_new)


def solution(mesh):
    return jax.shard_map(
        on_device,
        mesh=mesh,
        in_specs=(
            P(ALONG, ACROSS, CHAN, None),
            P(ALONG, ACROSS, CHAN),
            P(CHAN),
            P(CHAN),
            P(ALONG, ACROSS),
            P(),
        ),
        out_specs=(
            P(ALONG, ACROSS, None),
            P(ALONG, ACROSS, None),
            P(ALONG, ACROSS, None),
        ),
        check_vma=False,
    )
```

```python
import jax
import jax.numpy as jnp
from jax import lax
from jax.experimental import pallas as pl
from jax.experimental.pallas import tpu as pltpu
from jax.sharding import PartitionSpec as P

BLOCKS = (2, 2, 3, 3)
ALONG, ACROSS, CHAN = "along", "across", "chan"
S = 384
F32 = jnp.float32
VEC = (4, 8, S)
WIDE, BACK = (12, 2, 8, S), (8, 2, 8, S)


def params():
    return pltpu.CompilerParams(vmem_limit_bytes=16 * 1024 * 1024)


class Refs(dict):
    __getattr__ = dict.__getitem__


def call(kernel, outs, ins, scratch=()):
    vmem = pl.BlockSpec(memory_space=pltpu.VMEM)
    args, in_tree = jax.tree.flatten([*ins.values()])
    shapes, out_tree = jax.tree.flatten([*outs.values()], is_leaf=lambda v: isinstance(v, tuple))
    n, m = len(args), len(args) + len(shapes)

    def body(*refs):
        named = zip([*ins, *outs], in_tree.unflatten(refs[:n]) + out_tree.unflatten(refs[n:m]))
        kernel(Refs(named), *refs[m:])

    result = pl.pallas_call(
        body,
        out_shape=[jax.ShapeDtypeStruct(s, F32) for s in shapes],
        in_specs=[vmem] * len(args),
        out_specs=[vmem] * len(shapes),
        scratch_shapes=[pltpu.VMEM(s, F32) for s in scratch],
        compiler_params=params(),
    )(*args)
    return Refs(zip(outs, out_tree.unflatten(result)))


def back_through(g_ref, at, t):
    return jnp.concatenate(
        [
            jnp.sum(g_ref[at, :, 128 * n : 128 * (n + 1)] * t, axis=0, keepdims=True)
            for n in range(3)
        ],
        axis=1,
    )


def project(jac, field, wcol, flag, out):
    def row(i, carry):
        x8 = field[i]
        sums = []
        for j in range(8):
            y = jnp.sum(jac[i * 8 + j] * x8[j : j + 1, :], axis=1, keepdims=True)
            sums.append(back_through(jac, i * 8 + j, y * wcol[...]))
        out[i] = jnp.concatenate(sums, axis=0) * flag[i]
        return carry

    lax.fori_loop(0, 4, row, 0)


def column(row, size):
    lane = lax.broadcasted_iota(jnp.int32, (size, size), 1)
    sub = lax.broadcasted_iota(jnp.int32, (size, size), 0)
    return jnp.sum(jnp.where(lane == sub, jnp.broadcast_to(row, (size, size)), 0.0), axis=1, keepdims=True)


def prepare_kernel(place, inv, use, clear, coef, wcol, flag, ctl, coefs):
    wcol[...] = jnp.broadcast_to(column(inv[...] * use[...].astype(F32), 128), (128, 128))
    for i in range(4):
        flag[i] = jnp.broadcast_to(column(clear[i : i + 1, :].astype(F32), 8), (8, S))
    for n in range(3):
        ctl[n] = jnp.broadcast_to(place[n], (8, 128)).astype(F32)
    low = lax.broadcasted_iota(jnp.int32, (8, 128), 0) < 4
    right, left = (jnp.broadcast_to(place[n], (8, 128)) for n in (3, 4))
    ctl[3] = jnp.where(low, right, left).astype(F32)
    for n in range(25):
        coefs[n] = jnp.broadcast_to(coef[n : n + 1, :], (8, S))


def first_kernel(r):
    def row(i, carry):
        d8 = r.dep[i]
        sums = []
        for j in range(8):
            t = column(d8[j : j + 1, :], 128) * r.wcol[...]
            sums.append(back_through(r.jac, i * 8 + j, t))
        r.share[i] = jnp.concatenate(sums, axis=0) * r.flag[i]
        return carry

    lax.fori_loop(0, 4, row, 0)


def fold(v):
    s = (v[0] + v[1]) + (v[2] + v[3])
    return (s[:, :128] + s[:, 128:256]) + s[:, 256:]


def put(ref, at, v):
    for n in range(3):
        ref[at + n] = v[:, 128 * n : 128 * (n + 1)]


def get(ref, at):
    return jnp.concatenate([ref[at + n] for n in range(3)], axis=1)


def sum_kernel(r):
    total = (r.own[...] + r.far[...]) + (r.near[...] + r.other[...])
    r.total[...] = total
    for h in range(2):
        put(r.to_right, 3 * h, jnp.concatenate([total[2 * h][4:], total[2 * h + 1][4:]], axis=0))
        put(r.to_left, 3 * h, jnp.concatenate([total[2 * h][:4], total[2 * h + 1][:4]], axis=0))
    if "grams" in r:
        count = r.grams.shape[0]
        for n in range(count):
            g = r.grams[n]
            if n == count - 1:
                g = g + fold(r.uq[...] * total)
            r.scal[n] = g
            r.to_right[6 + n] = g
            r.to_left[6 + n] = g


def join_kernel(r):
    keep = r.ctl[3][:, :1]
    left, right = r.from_left, r.from_right
    for i in range(4):
        put(r.ext, 3 * i, r.total[i])
        h, k = 3 * (i // 2), 4 * (i % 2)
        side = jnp.concatenate([get(right, h)[k : k + 4], get(left, h)[k : k + 4]], axis=0)
        put(r.ext, 12 + 3 * i, jnp.where(keep > 0.5, side, 0.0))
    if "scal" in r:
        for n in range(r.scal.shape[0]):
            s = (r.scal[n] + r.opposite[n]) + (left[6 + n] + right[6 + n])
            r.ext[24 + n] = s
            r.plane[n] = s


def part_kernel(r):
    for n in range(r.part.shape[0]):
        r.part[n] = (r.facing[24 + n] + r.beside[n]) + r.opposite[n]


def shifted(mid, side, d):
    if d == 0:
        return mid, side
    if d > 0:
        return (
            jnp.concatenate([mid[d:], side[:d]], axis=0),
            jnp.concatenate([side[d:], mid[:d]], axis=0),
        )
    d = -d
    return (
        jnp.concatenate([side[8 - d :], mid[: 8 - d]], axis=0),
        jnp.concatenate([mid[8 - d :], side[: 8 - d]], axis=0),
    )


def stencil(r, wide, back, kw, kkw):
    ctl, coef = r.ctl, r.coef
    odd, up_ok, down_ok = ctl[0][:, :1] > 0.5, ctl[1][:, :1] > 0.5, ctl[2][:, :1] > 0.5
    for i in range(4):
        for part in range(2):
            at = 12 * part + 3 * i
            a, b = get(r.first, at), get(r.second, at)
            wide[i, part] = jnp.where(up_ok, jnp.where(odd, a, b), 0.0)
            wide[4 + i, part] = get(r.ext, at)
            wide[8 + i, part] = jnp.where(down_ok, jnp.where(odd, b, a), 0.0)
    side_ok = ctl[3][:, :1] > 0.5

    def back_row(i, carry):
        mid_sum = side_sum = 0.0
        for b in range(5):
            m = s = 0.0
            for a in range(5):
                c = coef[5 * a + b]
                m = m + c * wide[i + 4 - a, 0]
                s = s + c * wide[i + 4 - a, 1]
            m, s = shifted(m, s, 2 - b)
            mid_sum, side_sum = mid_sum + m, side_sum + s
        back[i, 0] = mid_sum
        back[i, 1] = jnp.where(side_ok, side_sum, 0.0)
        return carry

    lax.fori_loop(0, 8, back_row, 0)
    for i in range(2):
        for part in range(2):
            back[i, part] = jnp.where(up_ok, back[i, part], 0.0)
            back[6 + i, part] = jnp.where(down_ok, back[6 + i, part], 0.0)
    for i in range(4):
        kw[i] = back[i + 2, 0]

    def row(i, carry):
        total = 0.0
        for b in range(5):
            m = s = 0.0
            for a in range(5):
                c = coef[5 * a + b]
                m = m + c * back[i + a, 0]
                s = s + c * back[i + a, 1]
            total = total + shifted(m, s, b - 2)[0]
        kkw[i] = total
        return carry

    if kkw is not None:
        lax.fori_loop(0, 4, row, 0)


def start_kernel(r, wide, back):
    stencil(r, wide, back, r.u0, r.uq0)
    project(r.jac, r.uq0, r.wcol, r.flag, r.share)


def gram_rows(s, count):
    rows = [("t", k) for k in range(s)]
    rows += [("m", i, j) for i in range(s) for j in range(i, s) if i < s - 1]
    rows += [("x", n, k) for n in range(count) for k in range(s)]
    rows += [("f", n) for n in range(count)] + [("uu",)]
    return rows


def inner_kernel(k, s, count):
    def body(r, wide, back, kw, kkw):
        stencil(r, wide, back, kw, kkw)
        if "steer" in r:
            a, b = r.steer[0][:1, :1], r.steer[1][:1, :1]
        for basis, image, vector, q in ((r.us, r.image, r.u, kw), (r.uqs, r.imageq, r.uq, kkw)):
            v = basis[k - 1][...] + q[...]
            image[...] = v
            if "steer" in r:
                v = v - a * basis[k - 1][...]
                if k > 1:
                    v = v - b * basis[k - 2][...]
            vector[...] = v
        project(r.jac, r.uq, r.wcol, r.flag, r.share)
        if k < s - 1:
            return
        us, hus = [*r.us, r.u], [*r.hus, r.image]
        tiles = []
        for row in gram_rows(s, count):
            if row[0] == "t":
                x, y = us[row[1]][...], us[0][...]
            elif row[0] == "m":
                x, y = hus[row[1]][...], us[row[2]][...]
            elif row[0] == "x":
                x, y = r.hps[row[1]], us[row[2]][...]
            elif row[0] == "f":
                x, y = r.ps[row[1]], us[0][...]
            else:
                x, y = us[1][...], us[1][...]
            tiles.append(jnp.sum(fold(x * y), axis=0, keepdims=True))
        while len(tiles) % 8:
            tiles.append(jnp.zeros((1, 128), F32))
        for n in range(len(tiles) // 8):
            r.grams[n] = jnp.concatenate(tiles[8 * n : 8 * n + 8], axis=0)
        last = us[s - 1][...]
        r.grams[len(tiles) // 8] = fold(last * last)

    return body


def solve(scal, known, s, count, first):
    rows = gram_rows(s, count)
    packed = [jnp.sum(tile, axis=1, keepdims=True) for tile in scal[:-1]]
    val = {row: packed[n // 8][n % 8 : n % 8 + 1, :] for n, row in enumerate(rows)}
    w = {(i, j): val["m", i, j] for i in range(s) for j in range(i, s) if i < s - 1}
    w[s - 1, s - 1] = jnp.sum(scal[-1], axis=(0, 1), keepdims=True)
    y = [val["t", k] for k in range(s)]
    a = val["m", 0, 0] / y[0]
    b = (val["uu",] - y[1] * y[1] / y[0]) / y[0]
    inverse = [1.0 / known[n][:1, :1] for n in range(count)]
    old = [[val["x", n, k] * inverse[n] for k in range(s)] for n in range(count)]
    for n in range(count):
        for i in range(s):
            y[i] = y[i] - old[n][i] * val["f", n]
            for j in range(i, s):
                w[i, j] = w[i, j] - old[n][i] * val["x", n, j]
    new = {}
    for k in range(s):
        for i in range(k + 1, s):
            new[i, k] = w[k, i] / w[k, k]
        for i in range(k + 1, s):
            y[i] = y[i] - new[i, k] * y[k]
            for j in range(i, s):
                w[i, j] = w[i, j] - new[i, k] * w[k, j]
    fixes = [val["f", n] * inverse[n] for n in range(count)]
    pivots = [w[k, k] for k in range(s)]
    steps = [y[k] / w[k, k] for k in range(s)]
    return old, new, pivots, steps, fixes, (a, b if first else 0.5 * b)


def block_kernel(s, count, keep, first, final):
    def body(r, wide, back, kw, kkw):
        stencil(r, wide, back, kw, None if final else kkw)
        at = 24
        scal = [
            (r.ext[at + n] + r.first[at + n]) + (r.part[n] + r.mate[n])
            for n in range(r.part.shape[0])
        ]
        known = [r.known[n] for n in range(count)]
        old, new, pivots, steps, fixes, steer = solve(scal, known, s, count, first)

        def directions(stack, vectors):
            made = []
            for k, v in enumerate(vectors):
                for n in range(count):
                    v = v - old[n][k] * r.stacks[stack][n]
                for j in range(k):
                    v = v - new[k, j] * made[j]
                made.append(v)
            if not final:
                kept = [r.stacks[stack][n] for n in range(count)] + made
                for n, v in enumerate(kept[-keep:]):
                    r.stacks_new[stack][n] = v
            moved = steps[0] * made[0]
            for k in range(1, s):
                moved = moved + steps[k] * made[k]
            for n in range(count):
                moved = moved + fixes[n] * r.stacks[stack][n]
            return moved

        us, uqs, hus, huqs = ([v[...] for v in vs] for vs in (r.us, r.uqs, r.hus, r.huqs))
        moved = directions(0, us)
        r.x_new[...] = moved if first else r.x[...] + moved
        moved = directions(1, uqs)
        r.xq_new[...] = moved if first else r.xq[...] + moved
        r.r_new[...] = us[0] - directions(2, hus + [us[s - 1] + kw[...]])
        if final:
            return
        r.q_new[...] = uqs[0] - directions(3, huqs + [uqs[s - 1] + kkw[...]])
        kept = known + [jnp.broadcast_to(v, (8, 128)) for v in pivots]
        for n, v in enumerate(kept[-keep:]):
            r.known_new[n] = v
        for n, v in enumerate(steer):
            r.steer_new[n] = jnp.broadcast_to(v, (8, 128))
        project(r.jac, r.q_new, r.wcol, r.flag, r.share)

    return body


def move(x, axis, target):
    return lax.ppermute(x, axis, [(i, target(i)) for i in range(lax.axis_size(axis))])


def shift(x, axis, k):
    n = lax.axis_size(axis)
    return move(x, axis, lambda i: (i + k) % n)


def on_device(jacobian, departures, inv_variance, channel_use, clear_flags, coefficients):
    along, across = lax.axis_size(ALONG), lax.axis_size(ACROSS)
    a, c = lax.axis_index(ALONG), lax.axis_index(ACROSS)
    place = jnp.stack([a % 2, a > 0, a < along - 1, c < across - 1, c > 0]).astype(jnp.int32)
    vmem = pl.BlockSpec(memory_space=pltpu.VMEM)
    shapes = ((128, 128), VEC, (4, 8, 128), (25, 8, S), VEC)
    wcol, flag, ctl, coef = pl.pallas_call(
        prepare_kernel,
        out_shape=[
            jax.ShapeDtypeStruct(s, F32) for s in ((128, 128), VEC, (4, 8, 128), (25, 8, S))
        ],
        in_specs=[pl.BlockSpec(memory_space=pltpu.SMEM)] + [vmem] * 4,
        out_specs=[vmem] * 4,
        compiler_params=params(),
    )(place, inv_variance[None], channel_use[None], clear_flags, coefficients)
    jac = jacobian.reshape(32, 128, S)
    ins = dict(jac=jac, dep=departures, wcol=wcol, flag=flag)
    share = call(first_kernel, dict(share=VEC), ins).share
    consts = dict(ctl=ctl, coef=coef)
    sweep = dict(jac=jac, wcol=wcol, flag=flag)

    def exchange(share, sums=None):
        ins = dict(
            own=share,
            near=shift(share, CHAN, 1),
            far=shift(share, CHAN, 2),
            other=shift(share, CHAN, -1),
        )
        g = sums["grams"].shape[0] if sums else 0
        tail = (g, 8, 128)
        edge = (6 + g, 8, 128)
        outs = dict(total=VEC, to_right=edge, to_left=edge)
        if sums:
            ins |= sums
            outs |= dict(scal=tail)
        summed = call(sum_kernel, outs, ins)
        ins = dict(
            total=summed.total,
            from_left=shift(summed.to_right, ACROSS, 1),
            from_right=shift(summed.to_left, ACROSS, -1),
            ctl=ctl,
        )
        outs = dict(ext=(24 + g, 8, 128))
        if sums:
            ins |= dict(scal=summed.scal, opposite=shift(summed.scal, ACROSS, 2))
            outs |= dict(plane=tail)
        joined = call(join_kernel, outs, ins)
        ext = joined.ext
        near = dict(
            ext=ext,
            first=move(ext, ALONG, lambda i: i ^ 1),
            second=move(ext, ALONG, lambda i: (i - 1 if i % 2 == 0 else i + 1) % along),
        )
        if sums:
            plane = joined.plane
            ins = dict(
                facing=near["second"],
                beside=move(plane, ALONG, lambda i: (i + 2 if i % 2 == 0 else i - 2) % along),
                opposite=shift(plane, ALONG, 4),
            )
            part = call(part_kernel, dict(part=tail), ins).part
            near |= dict(part=part, mate=move(part, ALONG, lambda i: i ^ 1))
        return near | consts

    work = [WIDE, BACK]
    more = [WIDE, BACK, VEC, VEC]
    made = call(start_kernel, dict(u0=VEC, uq0=VEC, share=VEC), exchange(share) | sweep, work)
    us, uqs, hus, huqs = [made.u0], [made.uq0], [], []
    share = made.share
    state = old = steer = {}
    count = 0
    for number, s in enumerate(BLOCKS):
        final = number == len(BLOCKS) - 1
        for k in range(1, s):
            outs = dict(image=VEC, imageq=VEC, u=VEC, uq=VEC, share=VEC)
            ins = exchange(share) | sweep | steer | dict(us=us, uqs=uqs)
            if k == s - 1:
                outs |= dict(grams=(-(-len(gram_rows(s, count)) // 8) + 1, 8, 128))
                ins |= dict(hus=hus)
                if count:
                    ins |= dict(ps=old["stacks"][0], hps=old["stacks"][2])
            made = call(inner_kernel(k, s, count), outs, ins, more)
            share = made.share
            us, uqs = us + [made.u], uqs + [made.uq]
            hus, huqs = hus + [made.image], huqs + [made.imageq]
        near = exchange(share, dict(grams=made.grams, uq=made.uq))
        keep = 0 if final else min(count + s, BLOCKS[number + 1])
        ins = near | state | old | dict(us=us, uqs=uqs, hus=hus, huqs=huqs)
        outs = dict(x_new=VEC, xq_new=VEC, r_new=VEC)
        if not final:
            ins |= sweep
            outs |= dict(q_new=VEC, share=VEC, known_new=(keep, 8, 128), steer_new=(2, 8, 128))
            outs |= dict(stacks_new=[(keep, *VEC)] * 4)
        made = call(block_kernel(s, count, keep, number == 0, final), outs, ins, more)
        if final:
            return made.x_new, made.xq_new, made.r_new
        count = keep
        state = dict(x=made.x_new, xq=made.xq_new)
        us, uqs, hus, huqs = [made.r_new], [made.q_new], [], []
        share = made.share
        steer = dict(steer=made.steer_new)
        old = dict(known=made.known_new, stacks=made.stacks_new)


def solution(mesh):
    return jax.shard_map(
        on_device,
        mesh=mesh,
        in_specs=(
            P(ALONG, ACROSS, CHAN, None),
            P(ALONG, ACROSS, CHAN),
            P(CHAN),
            P(CHAN),
            P(ALONG, ACROSS),
            P(),
        ),
        out_specs=(
            P(ALONG, ACROSS, None),
            P(ALONG, ACROSS, None),
            P(ALONG, ACROSS, None),
        ),
        check_vma=False,
    )
```

```python
import jax
import jax.numpy as jnp
from jax import lax
from jax.experimental import pallas as pl
from jax.experimental.pallas import tpu as pltpu
from jax.sharding import PartitionSpec as P

STEPS = 3
LOOPS = 2
ALONG, ACROSS, CHAN = "along", "across", "chan"
S = 384
F32 = jnp.float32
VEC = (4, 8, S)
WIDE, BACK = (12, 2, 8, S), (8, 2, 8, S)


def params():
    return pltpu.CompilerParams(vmem_limit_bytes=16 * 1024 * 1024)


class Refs(dict):
    __getattr__ = dict.__getitem__


def leaves(tree):
    return [name for name, v in tree.items() for _ in (v if isinstance(v, list) else [v])]


def call(kernel, outs, ins, scratch=(), reuse=()):
    vmem = pl.BlockSpec(memory_space=pltpu.VMEM)
    args, in_tree = jax.tree.flatten([*ins.values()])
    shapes, out_tree = jax.tree.flatten([*outs.values()], is_leaf=lambda v: isinstance(v, tuple))
    n, m = len(args), len(args) + len(shapes)
    where = lambda tree, name: [k for k, path in enumerate(leaves(tree)) if path == name]
    aliases = {}
    for source, target in reuse:
        aliases |= dict(zip(where(ins, source), where(outs, target)))

    def body(*refs):
        named = zip([*ins, *outs], in_tree.unflatten(refs[:n]) + out_tree.unflatten(refs[n:m]))
        kernel(Refs(named), *refs[m:])

    result = pl.pallas_call(
        body,
        out_shape=[jax.ShapeDtypeStruct(s, F32) for s in shapes],
        in_specs=[vmem] * len(args),
        out_specs=[vmem] * len(shapes),
        scratch_shapes=[pltpu.VMEM(s, F32) for s in scratch],
        input_output_aliases=aliases,
        compiler_params=params(),
    )(*args)
    return Refs(zip(outs, out_tree.unflatten(result)))


def back_through(g_ref, at, t):
    return jnp.concatenate(
        [
            jnp.sum(g_ref[at, :, 128 * n : 128 * (n + 1)] * t, axis=0, keepdims=True)
            for n in range(3)
        ],
        axis=1,
    )


def project(jac, field, wcol, flag, out):
    def row(i, carry):
        x8 = field[i]
        sums = []
        for j in range(8):
            y = jnp.sum(jac[i * 8 + j] * x8[j : j + 1, :], axis=1, keepdims=True)
            sums.append(back_through(jac, i * 8 + j, y * wcol[...]))
        out[i] = jnp.concatenate(sums, axis=0) * flag[i]
        return carry

    lax.fori_loop(0, 4, row, 0)


def column(row, size):
    lane = lax.broadcasted_iota(jnp.int32, (size, size), 1)
    sub = lax.broadcasted_iota(jnp.int32, (size, size), 0)
    return jnp.sum(jnp.where(lane == sub, jnp.broadcast_to(row, (size, size)), 0.0), axis=1, keepdims=True)


def prepare_kernel(place, inv, use, clear, coef, wcol, flag, ctl, coefs):
    wcol[...] = jnp.broadcast_to(column(inv[...] * use[...].astype(F32), 128), (128, 128))
    for i in range(4):
        flag[i] = jnp.broadcast_to(column(clear[i : i + 1, :].astype(F32), 8), (8, S))
    for n in range(3):
        ctl[n] = jnp.broadcast_to(place[n], (8, 128)).astype(F32)
    low = lax.broadcasted_iota(jnp.int32, (8, 128), 0) < 4
    right, left = (jnp.broadcast_to(place[n], (8, 128)) for n in (3, 4))
    ctl[3] = jnp.where(low, right, left).astype(F32)
    for n in range(25):
        coefs[n] = jnp.broadcast_to(coef[n : n + 1, :], (8, S))


def first_kernel(r):
    def row(i, carry):
        d8 = r.dep[i]
        sums = []
        for j in range(8):
            t = column(d8[j : j + 1, :], 128) * r.wcol[...]
            sums.append(back_through(r.jac, i * 8 + j, t))
        r.share[i] = jnp.concatenate(sums, axis=0) * r.flag[i]
        return carry

    lax.fori_loop(0, 4, row, 0)


def fold(v):
    s = (v[0] + v[1]) + (v[2] + v[3])
    return (s[:, :128] + s[:, 128:256]) + s[:, 256:]


def put(ref, at, v):
    for n in range(3):
        ref[at + n] = v[:, 128 * n : 128 * (n + 1)]


def get(ref, at):
    return jnp.concatenate([ref[at + n] for n in range(3)], axis=1)


def sum_kernel(r):
    total = (r.own[...] + r.far[...]) + (r.near[...] + r.other[...])
    r.total[...] = total
    for h in range(2):
        put(r.to_right, 3 * h, jnp.concatenate([total[2 * h][4:], total[2 * h + 1][4:]], axis=0))
        put(r.to_left, 3 * h, jnp.concatenate([total[2 * h][:4], total[2 * h + 1][:4]], axis=0))
    if "grams" in r:
        count = r.grams.shape[0]
        for n in range(count):
            g = r.grams[n]
            if n == count - 1:
                g = g + fold(r.uq[...] * total)
            r.scal[n] = g
            r.to_right[6 + n] = g
            r.to_left[6 + n] = g


def join_kernel(r):
    keep = r.ctl[3][:, :1]
    left, right = r.from_left, r.from_right
    for i in range(4):
        put(r.ext, 3 * i, r.total[i])
        h, k = 3 * (i // 2), 4 * (i % 2)
        side = jnp.concatenate([get(right, h)[k : k + 4], get(left, h)[k : k + 4]], axis=0)
        put(r.ext, 12 + 3 * i, jnp.where(keep > 0.5, side, 0.0))
    if "scal" in r:
        for n in range(r.scal.shape[0]):
            s = (r.scal[n] + r.opposite[n]) + (left[6 + n] + right[6 + n])
            r.ext[24 + n] = s
            r.plane[n] = s


def part_kernel(r):
    for n in range(r.part.shape[0]):
        r.part[n] = (r.facing[24 + n] + r.beside[n]) + r.opposite[n]


def shifted(mid, side, d):
    if d == 0:
        return mid, side
    if d > 0:
        return (
            jnp.concatenate([mid[d:], side[:d]], axis=0),
            jnp.concatenate([side[d:], mid[:d]], axis=0),
        )
    d = -d
    return (
        jnp.concatenate([side[8 - d :], mid[: 8 - d]], axis=0),
        jnp.concatenate([mid[8 - d :], side[: 8 - d]], axis=0),
    )


def stencil(r, wide, back, kw, kkw):
    ctl, coef = r.ctl, r.coef
    odd, up_ok, down_ok = ctl[0][:, :1] > 0.5, ctl[1][:, :1] > 0.5, ctl[2][:, :1] > 0.5
    for i in range(4):
        for part in range(2):
            at = 12 * part + 3 * i
            a, b = get(r.first, at), get(r.second, at)
            wide[i, part] = jnp.where(up_ok, jnp.where(odd, a, b), 0.0)
            wide[4 + i, part] = get(r.ext, at)
            wide[8 + i, part] = jnp.where(down_ok, jnp.where(odd, b, a), 0.0)
    side_ok = ctl[3][:, :1] > 0.5

    def back_row(i, carry):
        mid_sum = side_sum = 0.0
        for b in range(5):
            m = s = 0.0
            for a in range(5):
                c = coef[5 * a + b]
                m = m + c * wide[i + 4 - a, 0]
                s = s + c * wide[i + 4 - a, 1]
            m, s = shifted(m, s, 2 - b)
            mid_sum, side_sum = mid_sum + m, side_sum + s
        back[i, 0] = mid_sum
        back[i, 1] = jnp.where(side_ok, side_sum, 0.0)
        return carry

    lax.fori_loop(0, 8, back_row, 0)
    for i in range(2):
        for part in range(2):
            back[i, part] = jnp.where(up_ok, back[i, part], 0.0)
            back[6 + i, part] = jnp.where(down_ok, back[6 + i, part], 0.0)
    for i in range(4):
        kw[i] = back[i + 2, 0]

    def row(i, carry):
        total = 0.0
        for b in range(5):
            m = s = 0.0
            for a in range(5):
                c = coef[5 * a + b]
                m = m + c * back[i + a, 0]
                s = s + c * back[i + a, 1]
            total = total + shifted(m, s, b - 2)[0]
        kkw[i] = total
        return carry

    if kkw is not None:
        lax.fori_loop(0, 4, row, 0)


def start_kernel(r, wide, back):
    stencil(r, wide, back, r.u0, r.uq0)
    project(r.jac, r.uq0, r.wcol, r.flag, r.share)
    u = r.u0[...]
    tile = fold(u * u)
    low = lax.broadcasted_iota(jnp.int32, (8, 128), 0) < 1
    r.grams[0] = jnp.where(low, jnp.sum(tile, axis=0, keepdims=True), 0.0)
    r.grams[1] = tile


def gram_rows(s, count):
    rows = [("t", k) for k in range(s)]
    rows += [("m", i, j) for i in range(s) for j in range(i, s) if i < s - 1]
    rows += [("x", n, k) for n in range(count) for k in range(s)]
    rows += [("f", n) for n in range(count)]
    return rows + [("uu",)] * (s > 1)


def inner_kernel(k, s, count):
    def body(r, wide, back, kw, kkw):
        stencil(r, wide, back, kw, kkw)
        if "steer" in r:
            a, b = r.steer[0][:1, :1], r.steer[1][:1, :1]
        for basis, image, vector, q in ((r.us, r.image, r.u, kw), (r.uqs, r.imageq, r.uq, kkw)):
            v = basis[k - 1][...] + q[...]
            image[...] = v
            if "steer" in r:
                v = v - a * basis[k - 1][...]
                if k > 1:
                    v = v - b * basis[k - 2][...]
            vector[...] = v
        project(r.jac, r.uq, r.wcol, r.flag, r.share)
        if k < s - 1:
            return
        us, hus = [*r.us, r.u], [*r.hus, r.image]
        tiles = []
        for row in gram_rows(s, count):
            if row[0] == "t":
                x, y = us[row[1]][...], us[0][...]
            elif row[0] == "m":
                x, y = hus[row[1]][...], us[row[2]][...]
            elif row[0] == "x":
                x, y = r.hps[row[1]], us[row[2]][...]
            elif row[0] == "f":
                x, y = r.ps[row[1]], us[0][...]
            else:
                x, y = us[1][...], us[1][...]
            tiles.append(jnp.sum(fold(x * y), axis=0, keepdims=True))
        while len(tiles) % 8:
            tiles.append(jnp.zeros((1, 128), F32))
        for n in range(len(tiles) // 8):
            r.grams[n] = jnp.concatenate(tiles[8 * n : 8 * n + 8], axis=0)
        last = us[s - 1][...]
        r.grams[len(tiles) // 8] = fold(last * last)

    return body


def solve(scal, known, s, count):
    rows = gram_rows(s, count)
    packed = [jnp.sum(tile, axis=1, keepdims=True) for tile in scal[:-1]]
    val = {row: packed[n // 8][n % 8 : n % 8 + 1, :] for n, row in enumerate(rows)}
    w = {(i, j): val["m", i, j] for i in range(s) for j in range(i, s) if i < s - 1}
    w[s - 1, s - 1] = jnp.sum(scal[-1], axis=(0, 1), keepdims=True)
    y = [val["t", k] for k in range(s)]
    a = w[0, 0] / y[0]
    b = 0.5 * (val["uu",] - y[1] * y[1] / y[0]) / y[0] if s > 1 else 0.25 * a * a
    inverse = [1.0 / known[n][:1, :1] for n in range(count)]
    old = [[val["x", n, k] * inverse[n] for k in range(s)] for n in range(count)]
    for n in range(count):
        for i in range(s):
            y[i] = y[i] - old[n][i] * val["f", n]
            for j in range(i, s):
                w[i, j] = w[i, j] - old[n][i] * val["x", n, j]
    new = {}
    for k in range(s):
        for i in range(k + 1, s):
            new[i, k] = w[k, i] / w[k, k]
        for i in range(k + 1, s):
            y[i] = y[i] - new[i, k] * y[k]
            for j in range(i, s):
                w[i, j] = w[i, j] - new[i, k] * w[k, j]
    fixes = [val["f", n] * inverse[n] for n in range(count)]
    pivots = [w[k, k] for k in range(s)]
    steps = [y[k] / w[k, k] for k in range(s)]
    return old, new, pivots, steps, fixes, (a, b)


def block_kernel(s, count, final):
    def body(r, wide, back, kw, kkw):
        stencil(r, wide, back, kw, None if final else kkw)
        at = 24
        scal = [
            (r.ext[at + n] + r.first[at + n]) + (r.part[n] + r.mate[n])
            for n in range(r.part.shape[0])
        ]
        known = [r.known[n] for n in range(count)]
        old, new, pivots, steps, fixes, steer = solve(scal, known, s, count)

        def directions(stack, vectors):
            lasts = [r.stacks[stack][n] for n in range(count)]
            made = []
            for k, v in enumerate(vectors):
                for n in range(count):
                    v = v - old[n][k] * lasts[n]
                for j in range(k):
                    v = v - new[k, j] * made[j]
                made.append(v)
            moved = steps[0] * made[0]
            for k in range(1, s):
                moved = moved + steps[k] * made[k]
            for n in range(count):
                moved = moved + fixes[n] * lasts[n]
            if not final:
                for n in range(STEPS):
                    r.stacks_new[stack][n] = made[n] if n < s else jnp.zeros(VEC, F32)
            return moved

        us, uqs, hus, huqs = ([v[...] for v in vs] for vs in (r.us, r.uqs, r.hus, r.huqs))
        moved = directions(0, us)
        r.x_new[...] = r.x[...] + moved if count else moved
        moved = directions(1, uqs)
        r.xq_new[...] = r.xq[...] + moved if count else moved
        r.r_new[...] = us[0] - directions(2, hus + [us[s - 1] + kw[...]])
        if final:
            return
        r.q_new[...] = uqs[0] - directions(3, huqs + [uqs[s - 1] + kkw[...]])
        for n in range(STEPS):
            v = pivots[n] if n < s else jnp.ones((1, 1), F32)
            r.known_new[n] = jnp.broadcast_to(v, (8, 128))
        for n, v in enumerate(steer):
            r.steer_new[n] = jnp.broadcast_to(v, (8, 128))
        project(r.jac, r.q_new, r.wcol, r.flag, r.share)

    return body


def move(x, axis, target):
    return lax.ppermute(x, axis, [(i, target(i)) for i in range(lax.axis_size(axis))])


def shift(x, axis, k):
    n = lax.axis_size(axis)
    return move(x, axis, lambda i: (i + k) % n)


def on_device(jacobian, departures, inv_variance, channel_use, clear_flags, coefficients):
    along, across = lax.axis_size(ALONG), lax.axis_size(ACROSS)
    a, c = lax.axis_index(ALONG), lax.axis_index(ACROSS)
    place = jnp.stack([a % 2, a > 0, a < along - 1, c < across - 1, c > 0]).astype(jnp.int32)
    vmem = pl.BlockSpec(memory_space=pltpu.VMEM)
    shapes = ((128, 128), VEC, (4, 8, 128), (25, 8, S), VEC)
    wcol, flag, ctl, coef = pl.pallas_call(
        prepare_kernel,
        out_shape=[
            jax.ShapeDtypeStruct(s, F32) for s in ((128, 128), VEC, (4, 8, 128), (25, 8, S))
        ],
        in_specs=[pl.BlockSpec(memory_space=pltpu.SMEM)] + [vmem] * 4,
        out_specs=[vmem] * 4,
        compiler_params=params(),
    )(place, inv_variance[None], channel_use[None], clear_flags, coefficients)
    jac = jacobian.reshape(32, 128, S)
    ins = dict(jac=jac, dep=departures, wcol=wcol, flag=flag)
    share = call(first_kernel, dict(share=VEC), ins).share
    consts = dict(ctl=ctl, coef=coef)
    sweep = dict(jac=jac, wcol=wcol, flag=flag)

    def exchange(share, sums=None):
        ins = dict(
            own=share,
            near=shift(share, CHAN, 1),
            far=shift(share, CHAN, 2),
            other=shift(share, CHAN, -1),
        )
        g = sums["grams"].shape[0] if sums else 0
        tail = (g, 8, 128)
        edge = (6 + g, 8, 128)
        outs = dict(total=VEC, to_right=edge, to_left=edge)
        if sums:
            ins |= sums
            outs |= dict(scal=tail)
        summed = call(sum_kernel, outs, ins)
        ins = dict(
            total=summed.total,
            from_left=shift(summed.to_right, ACROSS, 1),
            from_right=shift(summed.to_left, ACROSS, -1),
            ctl=ctl,
        )
        outs = dict(ext=(24 + g, 8, 128))
        if sums:
            ins |= dict(scal=summed.scal, opposite=shift(summed.scal, ACROSS, 2))
            outs |= dict(plane=tail)
        joined = call(join_kernel, outs, ins)
        ext = joined.ext
        near = dict(
            ext=ext,
            first=move(ext, ALONG, lambda i: i ^ 1),
            second=move(ext, ALONG, lambda i: (i - 1 if i % 2 == 0 else i + 1) % along),
        )
        if sums:
            plane = joined.plane
            ins = dict(
                facing=near["second"],
                beside=move(plane, ALONG, lambda i: (i + 2 if i % 2 == 0 else i - 2) % along),
                opposite=shift(plane, ALONG, 4),
            )
            part = call(part_kernel, dict(part=tail), ins).part
            near |= dict(part=part, mate=move(part, ALONG, lambda i: i ^ 1))
        return near | consts

    work = [WIDE, BACK]
    more = [WIDE, BACK, VEC, VEC]
    fresh = dict(
        q_new=VEC,
        share=VEC,
        known_new=(STEPS, 8, 128),
        steer_new=(2, 8, 128),
        stacks_new=[(STEPS, *VEC)] * 4,
    )

    def block(s, carry, final):
        share, r, q, state, steer, old, grams = carry
        count = STEPS if old else 0
        us, uqs, hus, huqs = [r], [q], [], []
        for k in range(1, s):
            outs = dict(image=VEC, imageq=VEC, u=VEC, uq=VEC, share=VEC)
            ins = exchange(share) | sweep | steer | dict(us=us, uqs=uqs)
            if k == s - 1:
                outs |= dict(grams=(-(-len(gram_rows(s, count)) // 8) + 1, 8, 128))
                ins |= dict(hus=hus, ps=old["stacks"][0], hps=old["stacks"][2])
            made = call(inner_kernel(k, s, count), outs, ins, more)
            share = made.share
            us, uqs = us + [made.u], uqs + [made.uq]
            hus, huqs = hus + [made.image], huqs + [made.imageq]
            if k == s - 1:
                grams = made.grams
        near = exchange(share, dict(grams=grams, uq=uqs[-1]))
        ins = near | state | old | steer | dict(us=us, uqs=uqs, hus=hus, huqs=huqs)
        outs = dict(x_new=VEC, xq_new=VEC, r_new=VEC)
        if final:
            made = call(block_kernel(s, count, True), outs, ins, more)
            return made.x_new, made.xq_new, made.r_new
        reuse = [(name, name + "_new") for name in (*state, *old, *steer)]
        made = call(block_kernel(s, count, False), outs | fresh, ins | sweep, more, reuse)
        state = dict(x=made.x_new, xq=made.xq_new)
        old = dict(known=made.known_new, stacks=made.stacks_new)
        return made.share, made.r_new, made.q_new, state, dict(steer=made.steer_new), old, None

    outs = dict(u0=VEC, uq0=VEC, share=VEC, grams=(2, 8, 128))
    made = call(start_kernel, outs, exchange(share) | sweep, work)
    carry = block(1, (made.share, made.u0, made.uq0, {}, {}, {}, made.grams), False)
    carry = lax.fori_loop(0, LOOPS, lambda i, c: block(STEPS, c, False), carry)
    return block(STEPS, carry, True)


def solution(mesh):
    return jax.shard_map(
        on_device,
        mesh=mesh,
        in_specs=(
            P(ALONG, ACROSS, CHAN, None),
            P(ALONG, ACROSS, CHAN),
            P(CHAN),
            P(CHAN),
            P(ALONG, ACROSS),
            P(),
        ),
        out_specs=(
            P(ALONG, ACROSS, None),
            P(ALONG, ACROSS, None),
            P(ALONG, ACROSS, None),
        ),
        check_vma=False,
    )
```

```python
import jax
import jax.numpy as jnp
from jax import lax
from jax.experimental import pallas as pl
from jax.experimental.pallas import tpu as pltpu
from jax.sharding import PartitionSpec as P

BLOCKS = (2, 3, 5)
ALONG, ACROSS, CHAN = "along", "across", "chan"
S = 384
F32 = jnp.float32
VEC = (4, 8, S)
WIDE, BACK = (12, 2, 8, S), (8, 2, 8, S)


def params():
    return pltpu.CompilerParams(vmem_limit_bytes=16 * 1024 * 1024)


class Refs(dict):
    __getattr__ = dict.__getitem__


def call(kernel, outs, ins, scratch=()):
    vmem = pl.BlockSpec(memory_space=pltpu.VMEM)
    args, in_tree = jax.tree.flatten([*ins.values()])
    shapes, out_tree = jax.tree.flatten([*outs.values()], is_leaf=lambda v: isinstance(v, tuple))
    n, m = len(args), len(args) + len(shapes)

    def body(*refs):
        named = zip([*ins, *outs], in_tree.unflatten(refs[:n]) + out_tree.unflatten(refs[n:m]))
        kernel(Refs(named), *refs[m:])

    result = pl.pallas_call(
        body,
        out_shape=[jax.ShapeDtypeStruct(s, F32) for s in shapes],
        in_specs=[vmem] * len(args),
        out_specs=[vmem] * len(shapes),
        scratch_shapes=[pltpu.VMEM(s, F32) for s in scratch],
        compiler_params=params(),
    )(*args)
    return Refs(zip(outs, out_tree.unflatten(result)))


def back_through(g_ref, at, t):
    return jnp.concatenate(
        [
            jnp.sum(g_ref[at, :, 128 * n : 128 * (n + 1)] * t, axis=0, keepdims=True)
            for n in range(3)
        ],
        axis=1,
    )


def project(jac, field, wcol, flag, out):
    def row(i, carry):
        x8 = field[i]
        sums = []
        for j in range(8):
            y = jnp.sum(jac[i * 8 + j] * x8[j : j + 1, :], axis=1, keepdims=True)
            sums.append(back_through(jac, i * 8 + j, y * wcol[...]))
        out[i] = jnp.concatenate(sums, axis=0) * flag[i]
        return carry

    lax.fori_loop(0, 4, row, 0)


def column(row, size):
    lane = lax.broadcasted_iota(jnp.int32, (size, size), 1)
    sub = lax.broadcasted_iota(jnp.int32, (size, size), 0)
    return jnp.sum(jnp.where(lane == sub, jnp.broadcast_to(row, (size, size)), 0.0), axis=1, keepdims=True)


def prepare_kernel(place, inv, use, clear, coef, wcol, flag, ctl, coefs):
    wcol[...] = jnp.broadcast_to(column(inv[...] * use[...].astype(F32), 128), (128, 128))
    for i in range(4):
        flag[i] = jnp.broadcast_to(column(clear[i : i + 1, :].astype(F32), 8), (8, S))
    for n in range(3):
        ctl[n] = jnp.broadcast_to(place[n], (8, 128)).astype(F32)
    low = lax.broadcasted_iota(jnp.int32, (8, 128), 0) < 4
    right, left = (jnp.broadcast_to(place[n], (8, 128)) for n in (3, 4))
    ctl[3] = jnp.where(low, right, left).astype(F32)
    for n in range(25):
        coefs[n] = jnp.broadcast_to(coef[n : n + 1, :], (8, S))


def first_kernel(r):
    def pair(h, carry):
        i, low = h // 4, 2 * (h % 4)
        for j in range(2):
            t = column(r.dep[i, pl.ds(low + j, 1)], 128) * r.wcol[...]
            r.share[i, pl.ds(low + j, 1)] = back_through(r.jac, 2 * h + j, t)
        return carry

    lax.fori_loop(0, 16, pair, 0)
    r.share[...] = r.share[...] * r.flag[...]


def fold(v):
    s = (v[0] + v[1]) + (v[2] + v[3])
    return (s[:, :128] + s[:, 128:256]) + s[:, 256:]


def put(ref, at, v):
    for n in range(3):
        ref[at + n] = v[:, 128 * n : 128 * (n + 1)]


def get(ref, at):
    return jnp.concatenate([ref[at + n] for n in range(3)], axis=1)


def sum_kernel(r):
    total = (r.own[...] + r.far[...]) + (r.near[...] + r.other[...])
    r.total[...] = total
    for h in range(2):
        put(r.to_right, 3 * h, jnp.concatenate([total[2 * h][4:], total[2 * h + 1][4:]], axis=0))
        put(r.to_left, 3 * h, jnp.concatenate([total[2 * h][:4], total[2 * h + 1][:4]], axis=0))
    if "grams" in r:
        count = r.grams.shape[0]
        for n in range(count):
            g = r.grams[n]
            if n == count - 1:
                g = g + fold(r.uq[...] * total)
            r.scal[n] = g
            r.to_right[6 + n] = g
            r.to_left[6 + n] = g


def join_kernel(r):
    keep = r.ctl[3][:, :1]
    left, right = r.from_left, r.from_right
    for i in range(4):
        put(r.ext, 3 * i, r.total[i])
        h, k = 3 * (i // 2), 4 * (i % 2)
        side = jnp.concatenate([get(right, h)[k : k + 4], get(left, h)[k : k + 4]], axis=0)
        put(r.ext, 12 + 3 * i, jnp.where(keep > 0.5, side, 0.0))
    if "scal" in r:
        for n in range(r.scal.shape[0]):
            s = (r.scal[n] + r.opposite[n]) + (left[6 + n] + right[6 + n])
            r.ext[24 + n] = s
            r.plane[n] = s


def part_kernel(r):
    for n in range(r.part.shape[0]):
        r.part[n] = (r.facing[24 + n] + r.beside[n]) + r.opposite[n]


def shifted(mid, side, d):
    if d == 0:
        return mid, side
    if d > 0:
        return (
            jnp.concatenate([mid[d:], side[:d]], axis=0),
            jnp.concatenate([side[d:], mid[:d]], axis=0),
        )
    d = -d
    return (
        jnp.concatenate([side[8 - d :], mid[: 8 - d]], axis=0),
        jnp.concatenate([mid[8 - d :], side[: 8 - d]], axis=0),
    )


def stencil(r, wide, back, kw, kkw):
    ctl, coef = r.ctl, r.coef
    odd, up_ok, down_ok = ctl[0][:, :1] > 0.5, ctl[1][:, :1] > 0.5, ctl[2][:, :1] > 0.5

    def lay(i, carry):
        for part in range(2):
            at = 12 * part + 3 * i
            a, b = get(r.first, at), get(r.second, at)
            wide[i, part] = jnp.where(up_ok, jnp.where(odd, a, b), 0.0)
            wide[4 + i, part] = get(r.ext, at)
            wide[8 + i, part] = jnp.where(down_ok, jnp.where(odd, b, a), 0.0)
        return carry

    lax.fori_loop(0, 4, lay, 0)
    side_ok = ctl[3][:, :1] > 0.5

    def back_row(i, carry):
        mid_sum = side_sum = 0.0
        for b in range(5):
            m = s = 0.0
            for a in range(5):
                c = coef[5 * a + b]
                m = m + c * wide[i + 4 - a, 0]
                s = s + c * wide[i + 4 - a, 1]
            m, s = shifted(m, s, 2 - b)
            mid_sum, side_sum = mid_sum + m, side_sum + s
        back[i, 0] = mid_sum
        back[i, 1] = jnp.where(side_ok, side_sum, 0.0)
        return carry

    lax.fori_loop(0, 8, back_row, 0)
    def edge(i, carry):
        for part in range(2):
            back[i, part] = jnp.where(up_ok, back[i, part], 0.0)
            back[6 + i, part] = jnp.where(down_ok, back[6 + i, part], 0.0)
        return carry

    lax.fori_loop(0, 2, edge, 0)
    for i in range(4):
        kw[i] = back[i + 2, 0]

    def row(i, carry):
        total = 0.0
        for b in range(5):
            m = s = 0.0
            for a in range(5):
                c = coef[5 * a + b]
                m = m + c * back[i + a, 0]
                s = s + c * back[i + a, 1]
            total = total + shifted(m, s, b - 2)[0]
        kkw[i] = total
        return carry

    if kkw is not None:
        lax.fori_loop(0, 4, row, 0)


def start_kernel(r, wide, back):
    stencil(r, wide, back, r.u0, r.uq0)
    project(r.jac, r.uq0, r.wcol, r.flag, r.share)


def gram_rows(s, count):
    rows = [("t", k) for k in range(s)]
    rows += [("m", i, j) for i in range(s) for j in range(i, s) if i < s - 1]
    rows += [("x", n, k) for n in range(count) for k in range(s)]
    rows += [("f", n) for n in range(count)] + [("uu",)]
    return rows


def inner_kernel(k, s, count):
    def body(r, wide, back, kw, kkw):
        stencil(r, wide, back, kw, kkw)
        if "steer" in r:
            a, b = r.steer[0][:1, :1], r.steer[1][:1, :1]
        for basis, image, vector, q in ((r.us, r.image, r.u, kw), (r.uqs, r.imageq, r.uq, kkw)):
            v = basis[k - 1][...] + q[...]
            image[...] = v
            if "steer" in r:
                v = v - a * basis[k - 1][...]
                if k > 1:
                    v = v - b * basis[k - 2][...]
            vector[...] = v
        project(r.jac, r.uq, r.wcol, r.flag, r.share)
        if k < s - 1:
            return
        us, hus = [*r.us, r.u], [*r.hus, r.image]
        tiles = []
        for row in gram_rows(s, count):
            if row[0] == "t":
                x, y = us[row[1]][...], us[0][...]
            elif row[0] == "m":
                x, y = hus[row[1]][...], us[row[2]][...]
            elif row[0] == "x":
                x, y = r.hps[row[1]], us[row[2]][...]
            elif row[0] == "f":
                x, y = r.ps[row[1]], us[0][...]
            else:
                x, y = us[1][...], us[1][...]
            tiles.append(jnp.sum(fold(x * y), axis=0, keepdims=True))
        while len(tiles) % 8:
            tiles.append(jnp.zeros((1, 128), F32))
        for n in range(len(tiles) // 8):
            r.grams[n] = jnp.concatenate(tiles[8 * n : 8 * n + 8], axis=0)
        last = us[s - 1][...]
        r.grams[len(tiles) // 8] = fold(last * last)

    return body


def solve(scal, known, s, count, first):
    rows = gram_rows(s, count)
    packed = [jnp.sum(tile, axis=1, keepdims=True) for tile in scal[:-1]]
    val = {row: packed[n // 8][n % 8 : n % 8 + 1, :] for n, row in enumerate(rows)}
    w = {(i, j): val["m", i, j] for i in range(s) for j in range(i, s) if i < s - 1}
    w[s - 1, s - 1] = jnp.sum(scal[-1], axis=(0, 1), keepdims=True)
    y = [val["t", k] for k in range(s)]
    a = (1.6 if first else 1.1) * val["m", 0, 0] / y[0]
    b = (2.0 if first else 0.6) * (val["uu",] - y[1] * y[1] / y[0]) / y[0]
    inverse = [1.0 / known[n][:1, :1] for n in range(count)]
    old = [[val["x", n, k] * inverse[n] for k in range(s)] for n in range(count)]
    for n in range(count):
        for i in range(s):
            y[i] = y[i] - old[n][i] * val["f", n]
            for j in range(i, s):
                w[i, j] = w[i, j] - old[n][i] * val["x", n, j]
    new = {}
    for k in range(s):
        for i in range(k + 1, s):
            new[i, k] = w[k, i] / w[k, k]
        for i in range(k + 1, s):
            y[i] = y[i] - new[i, k] * y[k]
            for j in range(i, s):
                w[i, j] = w[i, j] - new[i, k] * w[k, j]
    fixes = [val["f", n] * inverse[n] for n in range(count)]
    pivots = [w[k, k] for k in range(s)]
    steps = [y[k] / w[k, k] for k in range(s)]
    return old, new, pivots, steps, fixes, (a, b)


def block_kernel(s, count, keep, first, final):
    def body(r, wide, back, kw, kkw):
        stencil(r, wide, back, kw, None if final else kkw)
        at = 24
        scal = [
            (r.ext[at + n] + r.first[at + n]) + (r.part[n] + r.mate[n])
            for n in range(r.part.shape[0])
        ]
        known = [r.known[n] for n in range(count)]
        old, new, pivots, steps, fixes, steer = solve(scal, known, s, count, first)

        def directions(stack, vectors):
            made = []
            for k, v in enumerate(vectors):
                for n in range(count):
                    v = v - old[n][k] * r.stacks[stack][n]
                for j in range(k):
                    v = v - new[k, j] * made[j]
                made.append(v)
            if not final:
                kept = [r.stacks[stack][n] for n in range(count)] + made
                for n, v in enumerate(kept[-keep:]):
                    r.stacks_new[stack][n] = v
            moved = steps[0] * made[0]
            for k in range(1, s):
                moved = moved + steps[k] * made[k]
            for n in range(count):
                moved = moved + fixes[n] * r.stacks[stack][n]
            return moved

        us, uqs, hus, huqs = ([v[...] for v in vs] for vs in (r.us, r.uqs, r.hus, r.huqs))
        moved = directions(0, us)
        r.x_new[...] = moved if first else r.x[...] + moved
        moved = directions(1, uqs)
        r.xq_new[...] = moved if first else r.xq[...] + moved
        r.r_new[...] = us[0] - directions(2, hus + [us[s - 1] + kw[...]])
        if final:
            return
        r.q_new[...] = uqs[0] - directions(3, huqs + [uqs[s - 1] + kkw[...]])
        kept = known + [jnp.broadcast_to(v, (8, 128)) for v in pivots]
        for n, v in enumerate(kept[-keep:]):
            r.known_new[n] = v
        for n, v in enumerate(steer):
            r.steer_new[n] = jnp.broadcast_to(v, (8, 128))
        project(r.jac, r.q_new, r.wcol, r.flag, r.share)

    return body


def move(x, axis, target):
    return lax.ppermute(x, axis, [(i, target(i)) for i in range(lax.axis_size(axis))])


def shift(x, axis, k):
    n = lax.axis_size(axis)
    return move(x, axis, lambda i: (i + k) % n)


def on_device(jacobian, departures, inv_variance, channel_use, clear_flags, coefficients):
    along, across = lax.axis_size(ALONG), lax.axis_size(ACROSS)
    a, c = lax.axis_index(ALONG), lax.axis_index(ACROSS)
    place = jnp.stack([a % 2, a > 0, a < along - 1, c < across - 1, c > 0]).astype(jnp.int32)
    vmem = pl.BlockSpec(memory_space=pltpu.VMEM)
    shapes = ((128, 128), VEC, (4, 8, 128), (25, 8, S), VEC)
    wcol, flag, ctl, coef = pl.pallas_call(
        prepare_kernel,
        out_shape=[
            jax.ShapeDtypeStruct(s, F32) for s in ((128, 128), VEC, (4, 8, 128), (25, 8, S))
        ],
        in_specs=[pl.BlockSpec(memory_space=pltpu.SMEM)] + [vmem] * 4,
        out_specs=[vmem] * 4,
        compiler_params=params(),
    )(place, inv_variance[None], channel_use[None], clear_flags, coefficients)
    jac = jacobian.reshape(32, 128, S)
    ins = dict(jac=jac, dep=departures, wcol=wcol, flag=flag)
    share = call(first_kernel, dict(share=VEC), ins).share
    consts = dict(ctl=ctl, coef=coef)
    sweep = dict(jac=jac, wcol=wcol, flag=flag)

    def exchange(share, sums=None):
        ins = dict(
            own=share,
            near=shift(share, CHAN, 1),
            far=shift(share, CHAN, 2),
            other=shift(share, CHAN, -1),
        )
        g = sums["grams"].shape[0] if sums else 0
        tail = (g, 8, 128)
        edge = (6 + g, 8, 128)
        outs = dict(total=VEC, to_right=edge, to_left=edge)
        if sums:
            ins |= sums
            outs |= dict(scal=tail)
        summed = call(sum_kernel, outs, ins)
        ins = dict(
            total=summed.total,
            from_left=shift(summed.to_right, ACROSS, 1),
            from_right=shift(summed.to_left, ACROSS, -1),
            ctl=ctl,
        )
        outs = dict(ext=(24 + g, 8, 128))
        if sums:
            ins |= dict(scal=summed.scal, opposite=shift(summed.scal, ACROSS, 2))
            outs |= dict(plane=tail)
        joined = call(join_kernel, outs, ins)
        ext = joined.ext
        near = dict(
            ext=ext,
            first=move(ext, ALONG, lambda i: i ^ 1),
            second=move(ext, ALONG, lambda i: (i - 1 if i % 2 == 0 else i + 1) % along),
        )
        if sums:
            plane = joined.plane
            ins = dict(
                facing=near["second"],
                beside=move(plane, ALONG, lambda i: (i + 2 if i % 2 == 0 else i - 2) % along),
                opposite=shift(plane, ALONG, 4),
            )
            part = call(part_kernel, dict(part=tail), ins).part
            near |= dict(part=part, mate=move(part, ALONG, lambda i: i ^ 1))
        return near | consts

    work = [WIDE, BACK]
    more = [WIDE, BACK, VEC, VEC]
    made = call(start_kernel, dict(u0=VEC, uq0=VEC, share=VEC), exchange(share) | sweep, work)
    us, uqs, hus, huqs = [made.u0], [made.uq0], [], []
    share = made.share
    state = old = steer = {}
    count = 0
    for number, s in enumerate(BLOCKS):
        final = number == len(BLOCKS) - 1
        for k in range(1, s):
            outs = dict(image=VEC, imageq=VEC, u=VEC, uq=VEC, share=VEC)
            ins = exchange(share) | sweep | steer | dict(us=us, uqs=uqs)
            if k == s - 1:
                outs |= dict(grams=(-(-len(gram_rows(s, count)) // 8) + 1, 8, 128))
                ins |= dict(hus=hus)
                if count:
                    ins |= dict(ps=old["stacks"][0], hps=old["stacks"][2])
            made = call(inner_kernel(k, s, count), outs, ins, more)
            share = made.share
            us, uqs = us + [made.u], uqs + [made.uq]
            hus, huqs = hus + [made.image], huqs + [made.imageq]
        near = exchange(share, dict(grams=made.grams, uq=made.uq))
        keep = 0 if final else min(count + s, BLOCKS[number + 1])
        ins = near | state | old | dict(us=us, uqs=uqs, hus=hus, huqs=huqs)
        outs = dict(x_new=VEC, xq_new=VEC, r_new=VEC)
        if not final:
            ins |= sweep
            outs |= dict(q_new=VEC, share=VEC, known_new=(keep, 8, 128), steer_new=(2, 8, 128))
            outs |= dict(stacks_new=[(keep, *VEC)] * 4)
        made = call(block_kernel(s, count, keep, number == 0, final), outs, ins, more)
        if final:
            return made.x_new, made.xq_new, made.r_new
        count = keep
        state = dict(x=made.x_new, xq=made.xq_new)
        us, uqs, hus, huqs = [made.r_new], [made.q_new], [], []
        share = made.share
        steer = dict(steer=made.steer_new)
        old = dict(known=made.known_new, stacks=made.stacks_new)


def solution(mesh):
    return jax.shard_map(
        on_device,
        mesh=mesh,
        in_specs=(
            P(ALONG, ACROSS, CHAN, None),
            P(ALONG, ACROSS, CHAN),
            P(CHAN),
            P(CHAN),
            P(ALONG, ACROSS),
            P(),
        ),
        out_specs=(
            P(ALONG, ACROSS, None),
            P(ALONG, ACROSS, None),
            P(ALONG, ACROSS, None),
        ),
        check_vma=False,
    )
```

```python
import jax
import jax.numpy as jnp
from jax import lax
from jax.experimental import pallas as pl
from jax.experimental.pallas import tpu as pltpu
from jax.sharding import PartitionSpec as P

BLOCKS = (2, 3, 5)
ALONG, ACROSS, CHAN = "along", "across", "chan"
S = 384
F32 = jnp.float32
VEC = (4, 8, S)
WIDE, BACK = (12, 2, 8, S), (8, 2, 8, S)


def params():
    return pltpu.CompilerParams(vmem_limit_bytes=16 * 1024 * 1024)


class Refs(dict):
    __getattr__ = dict.__getitem__


def call(kernel, outs, ins, scratch=()):
    vmem = pl.BlockSpec(memory_space=pltpu.VMEM)
    args, in_tree = jax.tree.flatten([*ins.values()])
    shapes, out_tree = jax.tree.flatten([*outs.values()], is_leaf=lambda v: isinstance(v, tuple))
    n, m = len(args), len(args) + len(shapes)

    def body(*refs):
        named = zip([*ins, *outs], in_tree.unflatten(refs[:n]) + out_tree.unflatten(refs[n:m]))
        kernel(Refs(named), *refs[m:])

    result = pl.pallas_call(
        body,
        out_shape=[jax.ShapeDtypeStruct(s, F32) for s in shapes],
        in_specs=[vmem] * len(args),
        out_specs=[vmem] * len(shapes),
        scratch_shapes=[pltpu.VMEM(s, F32) for s in scratch],
        compiler_params=params(),
    )(*args)
    return Refs(zip(outs, out_tree.unflatten(result)))


def back_through(g_ref, at, t):
    return jnp.concatenate(
        [
            jnp.sum(g_ref[at, :, 128 * n : 128 * (n + 1)] * t, axis=0, keepdims=True)
            for n in range(3)
        ],
        axis=1,
    )


def project(jac, field, wcol, flag, out):
    def row(i, carry):
        x8 = field[i]
        sums = []
        for j in range(8):
            y = jnp.sum(jac[i * 8 + j] * x8[j : j + 1, :], axis=1, keepdims=True)
            sums.append(back_through(jac, i * 8 + j, y * wcol[...]))
        out[i] = jnp.concatenate(sums, axis=0) * flag[i]
        return carry

    lax.fori_loop(0, 4, row, 0)


def column(row, size):
    lane = lax.broadcasted_iota(jnp.int32, (size, size), 1)
    sub = lax.broadcasted_iota(jnp.int32, (size, size), 0)
    return jnp.sum(jnp.where(lane == sub, jnp.broadcast_to(row, (size, size)), 0.0), axis=1, keepdims=True)


def prepare_kernel(place, inv, use, clear, coef, wcol, flag, ctl, coefs):
    wcol[...] = jnp.broadcast_to(column(inv[...] * use[...].astype(F32), 128), (128, 128))
    for i in range(4):
        flag[i] = jnp.broadcast_to(column(clear[i : i + 1, :].astype(F32), 8), (8, S))
    for n in range(3):
        ctl[n] = jnp.broadcast_to(place[n], (8, 128)).astype(F32)
    low = lax.broadcasted_iota(jnp.int32, (8, 128), 0) < 4
    right, left = (jnp.broadcast_to(place[n], (8, 128)) for n in (3, 4))
    ctl[3] = jnp.where(low, right, left).astype(F32)
    for n in range(25):
        coefs[n] = jnp.broadcast_to(coef[n : n + 1, :], (8, S))


def first_kernel(r):
    def row(i, carry):
        d8 = r.dep[i]
        sums = []
        for j in range(8):
            t = column(d8[j : j + 1, :], 128) * r.wcol[...]
            sums.append(back_through(r.jac, i * 8 + j, t))
        r.share[i] = jnp.concatenate(sums, axis=0) * r.flag[i]
        return carry

    lax.fori_loop(0, 4, row, 0)


def fold(v):
    s = (v[0] + v[1]) + (v[2] + v[3])
    return (s[:, :128] + s[:, 128:256]) + s[:, 256:]


def put(ref, at, v):
    for n in range(3):
        ref[at + n] = v[:, 128 * n : 128 * (n + 1)]


def get(ref, at):
    return jnp.concatenate([ref[at + n] for n in range(3)], axis=1)


def sum_kernel(r):
    total = (r.own[...] + r.far[...]) + (r.near[...] + r.other[...])
    r.total[...] = total
    for h in range(2):
        put(r.to_right, 3 * h, jnp.concatenate([total[2 * h][4:], total[2 * h + 1][4:]], axis=0))
        put(r.to_left, 3 * h, jnp.concatenate([total[2 * h][:4], total[2 * h + 1][:4]], axis=0))
    if "grams" in r:
        count = r.grams.shape[0]
        for n in range(count):
            g = r.grams[n]
            if n == count - 1:
                g = g + fold(r.uq[...] * total)
            r.scal[n] = g
            r.to_right[6 + n] = g
            r.to_left[6 + n] = g


def join_kernel(r):
    keep = r.ctl[3][:, :1]
    left, right = r.from_left, r.from_right
    for i in range(4):
        put(r.ext, 3 * i, r.total[i])
        h, k = 3 * (i // 2), 4 * (i % 2)
        side = jnp.concatenate([get(right, h)[k : k + 4], get(left, h)[k : k + 4]], axis=0)
        put(r.ext, 12 + 3 * i, jnp.where(keep > 0.5, side, 0.0))
    if "scal" in r:
        for n in range(r.scal.shape[0]):
            s = (r.scal[n] + r.opposite[n]) + (left[6 + n] + right[6 + n])
            r.ext[24 + n] = s
            r.plane[n] = s


def part_kernel(r):
    for n in range(r.part.shape[0]):
        r.part[n] = (r.facing[24 + n] + r.beside[n]) + r.opposite[n]


def shifted(mid, side, d):
    if d == 0:
        return mid, side
    if d > 0:
        return (
            jnp.concatenate([mid[d:], side[:d]], axis=0),
            jnp.concatenate([side[d:], mid[:d]], axis=0),
        )
    d = -d
    return (
        jnp.concatenate([side[8 - d :], mid[: 8 - d]], axis=0),
        jnp.concatenate([mid[8 - d :], side[: 8 - d]], axis=0),
    )


def stencil(r, wide, back, kw, kkw):
    ctl, coef = r.ctl, r.coef
    odd, up_ok, down_ok = ctl[0][:, :1] > 0.5, ctl[1][:, :1] > 0.5, ctl[2][:, :1] > 0.5
    for i in range(4):
        for part in range(2):
            at = 12 * part + 3 * i
            a, b = get(r.first, at), get(r.second, at)
            wide[i, part] = jnp.where(up_ok, jnp.where(odd, a, b), 0.0)
            wide[4 + i, part] = get(r.ext, at)
            wide[8 + i, part] = jnp.where(down_ok, jnp.where(odd, b, a), 0.0)
    side_ok = ctl[3][:, :1] > 0.5

    def back_row(i, carry):
        mid_sum = side_sum = 0.0
        for b in range(5):
            m = s = 0.0
            for a in range(5):
                c = coef[5 * a + b]
                m = m + c * wide[i + 4 - a, 0]
                s = s + c * wide[i + 4 - a, 1]
            m, s = shifted(m, s, 2 - b)
            mid_sum, side_sum = mid_sum + m, side_sum + s
        back[i, 0] = mid_sum
        back[i, 1] = jnp.where(side_ok, side_sum, 0.0)
        return carry

    lax.fori_loop(0, 8, back_row, 0)
    for i in range(2):
        for part in range(2):
            back[i, part] = jnp.where(up_ok, back[i, part], 0.0)
            back[6 + i, part] = jnp.where(down_ok, back[6 + i, part], 0.0)
    for i in range(4):
        kw[i] = back[i + 2, 0]

    def row(i, carry):
        total = 0.0
        for b in range(5):
            m = s = 0.0
            for a in range(5):
                c = coef[5 * a + b]
                m = m + c * back[i + a, 0]
                s = s + c * back[i + a, 1] if b != 2 else s
            total = total + (shifted(m, s, b - 2)[0] if b != 2 else m)
        kkw[i] = total
        return carry

    if kkw is not None:
        lax.fori_loop(0, 4, row, 0)


def start_kernel(r, wide, back):
    stencil(r, wide, back, r.u0, r.uq0)
    project(r.jac, r.uq0, r.wcol, r.flag, r.share)


def gram_rows(s, count):
    rows = [("t", k) for k in range(s)]
    rows += [("m", i, j) for i in range(s) for j in range(i, s) if i < s - 1]
    rows += [("x", n, k) for n in range(count) for k in range(s)]
    rows += [("f", n) for n in range(count)] + [("uu",)]
    return rows


def inner_kernel(k, s, count):
    def body(r, wide, back, kw, kkw):
        stencil(r, wide, back, kw, kkw)
        if "steer" in r:
            a, b = r.steer[0][:1, :1], r.steer[1][:1, :1]
        for basis, image, vector, q in ((r.us, r.image, r.u, kw), (r.uqs, r.imageq, r.uq, kkw)):
            v = basis[k - 1][...] + q[...]
            image[...] = v
            if "steer" in r:
                v = v - a * basis[k - 1][...]
                if k > 1:
                    v = v - b * basis[k - 2][...]
            vector[...] = v
        project(r.jac, r.uq, r.wcol, r.flag, r.share)
        if k < s - 1:
            return
        us, hus = [*r.us, r.u], [*r.hus, r.image]
        tiles = []
        for row in gram_rows(s, count):
            if row[0] == "t":
                x, y = us[row[1]][...], us[0][...]
            elif row[0] == "m":
                x, y = hus[row[1]][...], us[row[2]][...]
            elif row[0] == "x":
                x, y = r.hps[row[1]], us[row[2]][...]
            elif row[0] == "f":
                x, y = r.ps[row[1]], us[0][...]
            else:
                x, y = us[1][...], us[1][...]
            tiles.append(jnp.sum(fold(x * y), axis=0, keepdims=True))
        while len(tiles) % 8:
            tiles.append(jnp.zeros((1, 128), F32))
        for n in range(len(tiles) // 8):
            r.grams[n] = jnp.concatenate(tiles[8 * n : 8 * n + 8], axis=0)
        last = us[s - 1][...]
        r.grams[len(tiles) // 8] = fold(last * last)

    return body


def solve(scal, known, s, count, first):
    rows = gram_rows(s, count)
    packed = [jnp.sum(tile, axis=1, keepdims=True) for tile in scal[:-1]]
    splat = lambda v: jnp.broadcast_to(v, (8, 128))
    val = {row: splat(packed[n // 8][n % 8 : n % 8 + 1, :]) for n, row in enumerate(rows)}
    w = {(i, j): val["m", i, j] for i in range(s) for j in range(i, s) if i < s - 1}
    w[s - 1, s - 1] = splat(jnp.sum(scal[-1], axis=(0, 1), keepdims=True))
    y = [val["t", k] for k in range(s)]
    a = (1.6 if first else 1.1) * val["m", 0, 0] / y[0]
    b = (2.0 if first else 0.6) * (val["uu",] - y[1] * y[1] / y[0]) / y[0]
    inverse = [1.0 / known[n] for n in range(count)]
    old = [[val["x", n, k] * inverse[n] for k in range(s)] for n in range(count)]
    for n in range(count):
        for i in range(s):
            y[i] = y[i] - old[n][i] * val["f", n]
            for j in range(i, s):
                w[i, j] = w[i, j] - old[n][i] * val["x", n, j]
    new = {}
    for k in range(s):
        for i in range(k + 1, s):
            new[i, k] = w[k, i] / w[k, k]
        for i in range(k + 1, s):
            y[i] = y[i] - new[i, k] * y[k]
            for j in range(i, s):
                w[i, j] = w[i, j] - new[i, k] * w[k, j]
    fixes = [val["f", n] * inverse[n] for n in range(count)]
    pivots = [w[k, k] for k in range(s)]
    steps = [y[k] / w[k, k] for k in range(s)]
    row = lambda v: jnp.concatenate([v] * 3, axis=1)
    old = [[row(v) for v in vs] for vs in old]
    new = {key: row(v) for key, v in new.items()}
    return old, new, pivots, [row(v) for v in steps], [row(v) for v in fixes], (a, b)


def block_kernel(s, count, keep, first, final):
    def body(r, wide, back, kw, kkw):
        stencil(r, wide, back, kw, None if final else kkw)
        at = 24
        scal = [
            (r.ext[at + n] + r.first[at + n]) + (r.part[n] + r.mate[n])
            for n in range(r.part.shape[0])
        ]
        known = [r.known[n] for n in range(count)]
        old, new, pivots, steps, fixes, steer = solve(scal, known, s, count, first)

        def directions(i, stack, vectors):
            lasts = [r.stacks[stack][n, i] for n in range(count)]
            made = []
            for k, v in enumerate(vectors):
                for n in range(count):
                    v = v - old[n][k] * lasts[n]
                for j in range(k):
                    v = v - new[k, j] * made[j]
                made.append(v)
            if not final:
                for n, v in enumerate((lasts + made)[-keep:]):
                    r.stacks_new[stack][n, i] = v
            moved = steps[0] * made[0]
            for k in range(1, s):
                moved = moved + steps[k] * made[k]
            for n in range(count):
                moved = moved + fixes[n] * lasts[n]
            return moved

        def row(i, carry):
            us, uqs, hus, huqs = ([v[i] for v in vs] for vs in (r.us, r.uqs, r.hus, r.huqs))
            moved = directions(i, 0, us)
            r.x_new[i] = moved if first else r.x[i] + moved
            moved = directions(i, 1, uqs)
            r.xq_new[i] = moved if first else r.xq[i] + moved
            r.r_new[i] = us[0] - directions(i, 2, hus + [us[s - 1] + kw[i]])
            if not final:
                r.q_new[i] = uqs[0] - directions(i, 3, huqs + [uqs[s - 1] + kkw[i]])
            return carry

        lax.fori_loop(0, 4, row, 0)
        if final:
            return
        for n, v in enumerate((known + pivots)[-keep:]):
            r.known_new[n] = v
        for n, v in enumerate(steer):
            r.steer_new[n] = v
        project(r.jac, r.q_new, r.wcol, r.flag, r.share)

    return body


def move(x, axis, target):
    return lax.ppermute(x, axis, [(i, target(i)) for i in range(lax.axis_size(axis))])


def shift(x, axis, k):
    n = lax.axis_size(axis)
    return move(x, axis, lambda i: (i + k) % n)


def on_device(jacobian, departures, inv_variance, channel_use, clear_flags, coefficients):
    along, across = lax.axis_size(ALONG), lax.axis_size(ACROSS)
    a, c = lax.axis_index(ALONG), lax.axis_index(ACROSS)
    place = jnp.stack([a % 2, a > 0, a < along - 1, c < across - 1, c > 0]).astype(jnp.int32)
    vmem = pl.BlockSpec(memory_space=pltpu.VMEM)
    wcol, flag, ctl, coef = pl.pallas_call(
        prepare_kernel,
        out_shape=[
            jax.ShapeDtypeStruct(s, F32) for s in ((128, 128), VEC, (4, 8, 128), (25, 8, S))
        ],
        in_specs=[pl.BlockSpec(memory_space=pltpu.SMEM)] + [vmem] * 4,
        out_specs=[vmem] * 4,
        compiler_params=params(),
    )(place, inv_variance[None], channel_use[None], clear_flags, coefficients)
    jac = jacobian.reshape(32, 128, S)
    ins = dict(jac=jac, dep=departures, wcol=wcol, flag=flag)
    share = call(first_kernel, dict(share=VEC), ins).share
    consts = dict(ctl=ctl, coef=coef)
    sweep = dict(jac=jac, wcol=wcol, flag=flag)

    def exchange(share, sums=None):
        ins = dict(
            own=share,
            near=shift(share, CHAN, 1),
            far=shift(share, CHAN, 2),
            other=shift(share, CHAN, -1),
        )
        g = sums["grams"].shape[0] if sums else 0
        tail = (g, 8, 128)
        edge = (6 + g, 8, 128)
        outs = dict(total=VEC, to_right=edge, to_left=edge)
        if sums:
            ins |= sums
            outs |= dict(scal=tail)
        summed = call(sum_kernel, outs, ins)
        ins = dict(
            total=summed.total,
            from_left=shift(summed.to_right, ACROSS, 1),
            from_right=shift(summed.to_left, ACROSS, -1),
            ctl=ctl,
        )
        outs = dict(ext=(24 + g, 8, 128))
        if sums:
            ins |= dict(scal=summed.scal, opposite=shift(summed.scal, ACROSS, 2))
            outs |= dict(plane=tail)
        joined = call(join_kernel, outs, ins)
        ext = joined.ext
        near = dict(
            ext=ext,
            first=move(ext, ALONG, lambda i: i ^ 1),
            second=move(ext, ALONG, lambda i: (i - 1 if i % 2 == 0 else i + 1) % along),
        )
        if sums:
            plane = joined.plane
            ins = dict(
                facing=near["second"],
                beside=move(plane, ALONG, lambda i: (i + 2 if i % 2 == 0 else i - 2) % along),
                opposite=shift(plane, ALONG, 4),
            )
            part = call(part_kernel, dict(part=tail), ins).part
            near |= dict(part=part, mate=move(part, ALONG, lambda i: i ^ 1))
        return near | consts

    work = [WIDE, BACK]
    more = [WIDE, BACK, VEC, VEC]
    made = call(start_kernel, dict(u0=VEC, uq0=VEC, share=VEC), exchange(share) | sweep, work)
    us, uqs, hus, huqs = [made.u0], [made.uq0], [], []
    share = made.share
    state = old = steer = {}
    count = 0
    for number, s in enumerate(BLOCKS):
        final = number == len(BLOCKS) - 1
        for k in range(1, s):
            outs = dict(image=VEC, imageq=VEC, u=VEC, uq=VEC, share=VEC)
            ins = exchange(share) | sweep | steer | dict(us=us, uqs=uqs)
            if k == s - 1:
                outs |= dict(grams=(-(-len(gram_rows(s, count)) // 8) + 1, 8, 128))
                ins |= dict(hus=hus)
                if count:
                    ins |= dict(ps=old["stacks"][0], hps=old["stacks"][2])
            made = call(inner_kernel(k, s, count), outs, ins, more)
            share = made.share
            us, uqs = us + [made.u], uqs + [made.uq]
            hus, huqs = hus + [made.image], huqs + [made.imageq]
        near = exchange(share, dict(grams=made.grams, uq=made.uq))
        keep = 0 if final else min(count + s, BLOCKS[number + 1])
        ins = near | state | old | dict(us=us, uqs=uqs, hus=hus, huqs=huqs)
        outs = dict(x_new=VEC, xq_new=VEC, r_new=VEC)
        if not final:
            ins |= sweep
            outs |= dict(q_new=VEC, share=VEC, known_new=(keep, 8, 128), steer_new=(2, 8, 128))
            outs |= dict(stacks_new=[(keep, *VEC)] * 4)
        made = call(block_kernel(s, count, keep, number == 0, final), outs, ins, more)
        if final:
            return made.x_new, made.xq_new, made.r_new
        count = keep
        state = dict(x=made.x_new, xq=made.xq_new)
        us, uqs, hus, huqs = [made.r_new], [made.q_new], [], []
        share = made.share
        steer = dict(steer=made.steer_new)
        old = dict(known=made.known_new, stacks=made.stacks_new)


def solution(mesh):
    return jax.shard_map(
        on_device,
        mesh=mesh,
        in_specs=(
            P(ALONG, ACROSS, CHAN, None),
            P(ALONG, ACROSS, CHAN),
            P(CHAN),
            P(CHAN),
            P(ALONG, ACROSS),
            P(),
        ),
        out_specs=(
            P(ALONG, ACROSS, None),
            P(ALONG, ACROSS, None),
            P(ALONG, ACROSS, None),
        ),
        check_vma=False,
    )
```

```python
import jax
import jax.numpy as jnp
from jax import lax
from jax.experimental import pallas as pl
from jax.experimental.pallas import tpu as pltpu
from jax.sharding import PartitionSpec as P

BLOCKS = (2, 3, 5)
ALONG, ACROSS, CHAN = "along", "across", "chan"
S = 384
F32 = jnp.float32
VEC = (4, 8, S)
WIDE, BACK = (12, 2, 8, S), (8, 2, 8, S)


def params():
    return pltpu.CompilerParams(vmem_limit_bytes=16 * 1024 * 1024)


class Refs(dict):
    __getattr__ = dict.__getitem__


def call(kernel, outs, ins, scratch=()):
    vmem = pl.BlockSpec(memory_space=pltpu.VMEM)
    args, in_tree = jax.tree.flatten([*ins.values()])
    shapes, out_tree = jax.tree.flatten([*outs.values()], is_leaf=lambda v: isinstance(v, tuple))
    n, m = len(args), len(args) + len(shapes)

    def body(*refs):
        named = zip([*ins, *outs], in_tree.unflatten(refs[:n]) + out_tree.unflatten(refs[n:m]))
        kernel(Refs(named), *refs[m:])

    result = pl.pallas_call(
        body,
        out_shape=[jax.ShapeDtypeStruct(s, F32) for s in shapes],
        in_specs=[vmem] * len(args),
        out_specs=[vmem] * len(shapes),
        scratch_shapes=[pltpu.VMEM(s, F32) for s in scratch],
        compiler_params=params(),
    )(*args)
    return Refs(zip(outs, out_tree.unflatten(result)))


def back_through(g_ref, at, t):
    return jnp.concatenate(
        [
            jnp.sum(g_ref[at, :, 128 * n : 128 * (n + 1)] * t, axis=0, keepdims=True)
            for n in range(3)
        ],
        axis=1,
    )


def project(jac, field, wcol, flag, out):
    def row(i, carry):
        x8 = field[i]
        sums = []
        for j in range(8):
            y = jnp.sum(jac[i * 8 + j] * x8[j : j + 1, :], axis=1, keepdims=True)
            sums.append(back_through(jac, i * 8 + j, y * wcol[...]))
        out[i] = jnp.concatenate(sums, axis=0) * flag[i]
        return carry

    lax.fori_loop(0, 4, row, 0)


def column(row, size):
    lane = lax.broadcasted_iota(jnp.int32, (size, size), 1)
    sub = lax.broadcasted_iota(jnp.int32, (size, size), 0)
    return jnp.sum(jnp.where(lane == sub, jnp.broadcast_to(row, (size, size)), 0.0), axis=1, keepdims=True)


def first_kernel(
    place, jac_hbm, dep_hbm, inv_hbm, use_hbm, clear_hbm, coef_hbm,
    jac, wcol, flag, ctl, coefs, share, dep, inv, use, clear, coef, sems,
):
    pairs = [(inv_hbm, inv), (use_hbm, use), (clear_hbm, clear), (coef_hbm, coef), (dep_hbm, dep)]
    pairs += [(jac_hbm.at[pl.ds(8 * i, 8)], jac.at[pl.ds(8 * i, 8)]) for i in range(4)]
    copies = [pltpu.make_async_copy(*pair, sems.at[n]) for n, pair in enumerate(pairs)]
    for copy in copies:
        copy.start()
    for n in range(3):
        ctl[n] = jnp.broadcast_to(place[n], (8, 128)).astype(F32)
    low = lax.broadcasted_iota(jnp.int32, (8, 128), 0) < 4
    right, left = (jnp.broadcast_to(place[n], (8, 128)) for n in (3, 4))
    ctl[3] = jnp.where(low, right, left).astype(F32)
    for copy in copies[:5]:
        copy.wait()
    wcol[...] = jnp.broadcast_to(column(inv[...] * use[...].astype(F32), 128), (128, 128))
    for i in range(4):
        flag[i] = jnp.broadcast_to(column(clear[i : i + 1, :].astype(F32), 8), (8, S))
    for n in range(25):
        coefs[n] = jnp.broadcast_to(coef[n : n + 1, :], (8, S))

    def row(i, carry):
        pltpu.make_async_copy(
            jac_hbm.at[pl.ds(8 * i, 8)], jac.at[pl.ds(8 * i, 8)], sems.at[5 + i]
        ).wait()
        d8 = dep[i]
        sums = []
        for j in range(8):
            t = column(d8[j : j + 1, :], 128) * wcol[...]
            sums.append(back_through(jac, i * 8 + j, t))
        share[i] = jnp.concatenate(sums, axis=0) * flag[i]
        return carry

    lax.fori_loop(0, 4, row, 0)


def fold(v):
    s = (v[0] + v[1]) + (v[2] + v[3])
    return (s[:, :128] + s[:, 128:256]) + s[:, 256:]


def put(ref, at, v):
    for n in range(3):
        ref[at + n] = v[:, 128 * n : 128 * (n + 1)]


def get(ref, at):
    return jnp.concatenate([ref[at + n] for n in range(3)], axis=1)


def sum_kernel(r):
    total = (r.own[...] + r.far[...]) + (r.near[...] + r.other[...])
    r.total[...] = total
    for h in range(2):
        put(r.to_right, 3 * h, jnp.concatenate([total[2 * h][4:], total[2 * h + 1][4:]], axis=0))
        put(r.to_left, 3 * h, jnp.concatenate([total[2 * h][:4], total[2 * h + 1][:4]], axis=0))
    if "grams" in r:
        count = r.grams.shape[0]
        for n in range(count):
            g = r.grams[n]
            if n == count - 1:
                g = g + fold(r.uq[...] * total)
            r.scal[n] = g
            r.to_right[6 + n] = g
            r.to_left[6 + n] = g


def join_kernel(r):
    keep = r.ctl[3][:, :1]
    left, right = r.from_left, r.from_right
    for i in range(4):
        put(r.ext, 3 * i, r.total[i])
        h, k = 3 * (i // 2), 4 * (i % 2)
        side = jnp.concatenate([get(right, h)[k : k + 4], get(left, h)[k : k + 4]], axis=0)
        put(r.ext, 12 + 3 * i, jnp.where(keep > 0.5, side, 0.0))
    if "scal" in r:
        for n in range(r.scal.shape[0]):
            s = (r.scal[n] + r.opposite[n]) + (left[6 + n] + right[6 + n])
            r.ext[24 + n] = s
            r.plane[n] = s


def part_kernel(r):
    for n in range(r.part.shape[0]):
        r.part[n] = (r.facing[24 + n] + r.beside[n]) + r.opposite[n]


def shifted(mid, side, d):
    if d == 0:
        return mid, side
    if d > 0:
        return (
            jnp.concatenate([mid[d:], side[:d]], axis=0),
            jnp.concatenate([side[d:], mid[:d]], axis=0),
        )
    d = -d
    return (
        jnp.concatenate([side[8 - d :], mid[: 8 - d]], axis=0),
        jnp.concatenate([mid[8 - d :], side[: 8 - d]], axis=0),
    )


def stencil(r, wide, back, kw, kkw):
    ctl, coef = r.ctl, r.coef
    odd, up_ok, down_ok = ctl[0][:, :1] > 0.5, ctl[1][:, :1] > 0.5, ctl[2][:, :1] > 0.5
    for i in range(4):
        for part in range(2):
            at = 12 * part + 3 * i
            a, b = get(r.first, at), get(r.second, at)
            wide[i, part] = jnp.where(up_ok, jnp.where(odd, a, b), 0.0)
            wide[4 + i, part] = get(r.ext, at)
            wide[8 + i, part] = jnp.where(down_ok, jnp.where(odd, b, a), 0.0)
    side_ok = ctl[3][:, :1] > 0.5

    def back_row(i, carry):
        mid_sum = side_sum = 0.0
        for b in range(5):
            m = s = 0.0
            for a in range(5):
                c = coef[5 * a + b]
                m = m + c * wide[i + 4 - a, 0]
                s = s + c * wide[i + 4 - a, 1]
            m, s = shifted(m, s, 2 - b)
            mid_sum, side_sum = mid_sum + m, side_sum + s
        back[i, 0] = mid_sum
        back[i, 1] = jnp.where(side_ok, side_sum, 0.0)
        return carry

    lax.fori_loop(0, 8, back_row, 0)
    for i in range(2):
        for part in range(2):
            back[i, part] = jnp.where(up_ok, back[i, part], 0.0)
            back[6 + i, part] = jnp.where(down_ok, back[6 + i, part], 0.0)
    for i in range(4):
        kw[i] = back[i + 2, 0]

    def row(i, carry):
        total = 0.0
        for b in range(5):
            m = s = 0.0
            for a in range(5):
                c = coef[5 * a + b]
                m = m + c * back[i + a, 0]
                s = s + c * back[i + a, 1] if b != 2 else s
            total = total + (shifted(m, s, b - 2)[0] if b != 2 else m)
        kkw[i] = total
        return carry

    if kkw is not None:
        lax.fori_loop(0, 4, row, 0)


def start_kernel(r, wide, back):
    stencil(r, wide, back, r.u0, r.uq0)
    project(r.jac, r.uq0, r.wcol, r.flag, r.share)


def gram_rows(s, count):
    rows = [("t", k) for k in range(s)]
    rows += [("m", i, j) for i in range(s) for j in range(i, s) if i < s - 1]
    rows += [("x", n, k) for n in range(count) for k in range(s)]
    rows += [("f", n) for n in range(count)] + [("uu",)]
    return rows


def inner_kernel(k, s, count):
    def body(r, wide, back, kw, kkw):
        stencil(r, wide, back, kw, kkw)
        if "steer" in r:
            a, b = r.steer[0][:1, :1], r.steer[1][:1, :1]
        for basis, image, vector, q in ((r.us, r.image, r.u, kw), (r.uqs, r.imageq, r.uq, kkw)):
            v = basis[k - 1][...] + q[...]
            image[...] = v
            if "steer" in r:
                v = v - a * basis[k - 1][...]
                if k > 1:
                    v = v - b * basis[k - 2][...]
            vector[...] = v
        project(r.jac, r.uq, r.wcol, r.flag, r.share)
        if k < s - 1:
            return
        us, hus = [*r.us, r.u], [*r.hus, r.image]
        tiles = []
        for row in gram_rows(s, count):
            if row[0] == "t":
                x, y = us[row[1]][...], us[0][...]
            elif row[0] == "m":
                x, y = hus[row[1]][...], us[row[2]][...]
            elif row[0] == "x":
                x, y = r.hps[row[1]], us[row[2]][...]
            elif row[0] == "f":
                x, y = r.ps[row[1]], us[0][...]
            else:
                x, y = us[1][...], us[1][...]
            tiles.append(jnp.sum(fold(x * y), axis=0, keepdims=True))
        while len(tiles) % 8:
            tiles.append(jnp.zeros((1, 128), F32))
        for n in range(len(tiles) // 8):
            r.grams[n] = jnp.concatenate(tiles[8 * n : 8 * n + 8], axis=0)
        last = us[s - 1][...]
        r.grams[len(tiles) // 8] = fold(last * last)

    return body


def solve(scal, known, s, count, first):
    rows = gram_rows(s, count)
    packed = [jnp.sum(tile, axis=1, keepdims=True) for tile in scal[:-1]]
    splat = lambda v: jnp.broadcast_to(v, (8, 128))
    val = {row: splat(packed[n // 8][n % 8 : n % 8 + 1, :]) for n, row in enumerate(rows)}
    w = {(i, j): val["m", i, j] for i in range(s) for j in range(i, s) if i < s - 1}
    w[s - 1, s - 1] = splat(jnp.sum(scal[-1], axis=(0, 1), keepdims=True))
    y = [val["t", k] for k in range(s)]
    a = (1.6 if first else 1.1) * val["m", 0, 0] / y[0]
    b = (2.0 if first else 0.6) * (val["uu",] - y[1] * y[1] / y[0]) / y[0]
    inverse = [1.0 / known[n] for n in range(count)]
    old = [[val["x", n, k] * inverse[n] for k in range(s)] for n in range(count)]
    for n in range(count):
        for i in range(s):
            y[i] = y[i] - old[n][i] * val["f", n]
            for j in range(i, s):
                w[i, j] = w[i, j] - old[n][i] * val["x", n, j]
    new = {}
    for k in range(s):
        for i in range(k + 1, s):
            new[i, k] = w[k, i] / w[k, k]
        for i in range(k + 1, s):
            y[i] = y[i] - new[i, k] * y[k]
            for j in range(i, s):
                w[i, j] = w[i, j] - new[i, k] * w[k, j]
    fixes = [val["f", n] * inverse[n] for n in range(count)]
    pivots = [w[k, k] for k in range(s)]
    steps = [y[k] / w[k, k] for k in range(s)]
    row = lambda v: jnp.concatenate([v] * 3, axis=1)
    old = [[row(v) for v in vs] for vs in old]
    new = {key: row(v) for key, v in new.items()}
    return old, new, pivots, [row(v) for v in steps], [row(v) for v in fixes], (a, b)


def block_kernel(s, count, keep, first, final):
    def body(r, wide, back, kw, kkw):
        stencil(r, wide, back, kw, None if final else kkw)
        at = 24
        scal = [
            (r.ext[at + n] + r.first[at + n]) + (r.part[n] + r.mate[n])
            for n in range(r.part.shape[0])
        ]
        known = [r.known[n] for n in range(count)]
        old, new, pivots, steps, fixes, steer = solve(scal, known, s, count, first)

        def directions(i, stack, vectors):
            lasts = [r.stacks[stack][n, i] for n in range(count)]
            made = []
            for k, v in enumerate(vectors):
                for n in range(count):
                    v = v - old[n][k] * lasts[n]
                for j in range(k):
                    v = v - new[k, j] * made[j]
                made.append(v)
            if not final:
                for n, v in enumerate((lasts + made)[-keep:]):
                    r.stacks_new[stack][n, i] = v
            moved = steps[0] * made[0]
            for k in range(1, s):
                moved = moved + steps[k] * made[k]
            for n in range(count):
                moved = moved + fixes[n] * lasts[n]
            return moved

        def row(i, carry):
            us, uqs, hus, huqs = ([v[i] for v in vs] for vs in (r.us, r.uqs, r.hus, r.huqs))
            moved = directions(i, 0, us)
            r.x_new[i] = moved if first else r.x[i] + moved
            moved = directions(i, 1, uqs)
            r.xq_new[i] = moved if first else r.xq[i] + moved
            r.r_new[i] = us[0] - directions(i, 2, hus + [us[s - 1] + kw[i]])
            if not final:
                r.q_new[i] = uqs[0] - directions(i, 3, huqs + [uqs[s - 1] + kkw[i]])
            return carry

        lax.fori_loop(0, 4, row, 0)
        if final:
            return
        for n, v in enumerate((known + pivots)[-keep:]):
            r.known_new[n] = v
        for n, v in enumerate(steer):
            r.steer_new[n] = v
        project(r.jac, r.q_new, r.wcol, r.flag, r.share)

    return body


def move(x, axis, target):
    return lax.ppermute(x, axis, [(i, target(i)) for i in range(lax.axis_size(axis))])


def shift(x, axis, k):
    n = lax.axis_size(axis)
    return move(x, axis, lambda i: (i + k) % n)


def on_device(jacobian, departures, inv_variance, channel_use, clear_flags, coefficients):
    along, across = lax.axis_size(ALONG), lax.axis_size(ACROSS)
    a, c = lax.axis_index(ALONG), lax.axis_index(ACROSS)
    place = jnp.stack([a % 2, a > 0, a < along - 1, c < across - 1, c > 0]).astype(jnp.int32)
    vmem = pl.BlockSpec(memory_space=pltpu.VMEM)
    shapes = ((32, 128, S), (128, 128), VEC, (4, 8, 128), (25, 8, S), VEC)
    here = [((4, 8, 128), F32), ((1, 128), F32), ((1, 128), jnp.int32), ((4, 8), jnp.int32), ((25, S), F32)]
    jac, wcol, flag, ctl, coef, share = pl.pallas_call(
        first_kernel,
        out_shape=[pltpu.VMEM(shapes[0], F32)] + [jax.ShapeDtypeStruct(s, F32) for s in shapes[1:]],
        in_specs=[pl.BlockSpec(memory_space=pltpu.SMEM)] + [pl.BlockSpec(memory_space=pl.ANY)] * 6,
        out_specs=[vmem] * 6,
        scratch_shapes=[pltpu.VMEM(*v) for v in here] + [pltpu.SemaphoreType.DMA((9,))],
        compiler_params=pltpu.CompilerParams(vmem_limit_bytes=48 * 1024 * 1024),
    )(
        place,
        jacobian.reshape(32, 128, S),
        departures,
        inv_variance[None],
        channel_use[None],
        clear_flags,
        coefficients,
    )
    consts = dict(ctl=ctl, coef=coef)
    sweep = dict(jac=jac, wcol=wcol, flag=flag)

    def exchange(share, sums=None):
        ins = dict(
            own=share,
            near=shift(share, CHAN, 1),
            far=shift(share, CHAN, 2),
            other=shift(share, CHAN, -1),
        )
        g = sums["grams"].shape[0] if sums else 0
        tail = (g, 8, 128)
        edge = (6 + g, 8, 128)
        outs = dict(total=VEC, to_right=edge, to_left=edge)
        if sums:
            ins |= sums
            outs |= dict(scal=tail)
        summed = call(sum_kernel, outs, ins)
        ins = dict(
            total=summed.total,
            from_left=shift(summed.to_right, ACROSS, 1),
            from_right=shift(summed.to_left, ACROSS, -1),
            ctl=ctl,
        )
        outs = dict(ext=(24 + g, 8, 128))
        if sums:
            ins |= dict(scal=summed.scal, opposite=shift(summed.scal, ACROSS, 2))
            outs |= dict(plane=tail)
        joined = call(join_kernel, outs, ins)
        ext = joined.ext
        near = dict(
            ext=ext,
            first=move(ext, ALONG, lambda i: i ^ 1),
            second=move(ext, ALONG, lambda i: (i - 1 if i % 2 == 0 else i + 1) % along),
        )
        if sums:
            plane = joined.plane
            ins = dict(
                facing=near["second"],
                beside=move(plane, ALONG, lambda i: (i + 2 if i % 2 == 0 else i - 2) % along),
                opposite=shift(plane, ALONG, 4),
            )
            part = call(part_kernel, dict(part=tail), ins).part
            near |= dict(part=part, mate=move(part, ALONG, lambda i: i ^ 1))
        return near | consts

    work = [WIDE, BACK]
    more = [WIDE, BACK, VEC, VEC]
    made = call(start_kernel, dict(u0=VEC, uq0=VEC, share=VEC), exchange(share) | sweep, work)
    us, uqs, hus, huqs = [made.u0], [made.uq0], [], []
    share = made.share
    state = old = steer = {}
    count = 0
    for number, s in enumerate(BLOCKS):
        final = number == len(BLOCKS) - 1
        for k in range(1, s):
            outs = dict(image=VEC, imageq=VEC, u=VEC, uq=VEC, share=VEC)
            ins = exchange(share) | sweep | steer | dict(us=us, uqs=uqs)
            if k == s - 1:
                outs |= dict(grams=(-(-len(gram_rows(s, count)) // 8) + 1, 8, 128))
                ins |= dict(hus=hus)
                if count:
                    ins |= dict(ps=old["stacks"][0], hps=old["stacks"][2])
            made = call(inner_kernel(k, s, count), outs, ins, more)
            share = made.share
            us, uqs = us + [made.u], uqs + [made.uq]
            hus, huqs = hus + [made.image], huqs + [made.imageq]
        near = exchange(share, dict(grams=made.grams, uq=made.uq))
        keep = 0 if final else min(count + s, BLOCKS[number + 1])
        ins = near | state | old | dict(us=us, uqs=uqs, hus=hus, huqs=huqs)
        outs = dict(x_new=VEC, xq_new=VEC, r_new=VEC)
        if not final:
            ins |= sweep
            outs |= dict(q_new=VEC, share=VEC, known_new=(keep, 8, 128), steer_new=(2, 8, 128))
            outs |= dict(stacks_new=[(keep, *VEC)] * 4)
        made = call(block_kernel(s, count, keep, number == 0, final), outs, ins, more)
        if final:
            return made.x_new, made.xq_new, made.r_new
        count = keep
        state = dict(x=made.x_new, xq=made.xq_new)
        us, uqs, hus, huqs = [made.r_new], [made.q_new], [], []
        share = made.share
        steer = dict(steer=made.steer_new)
        old = dict(known=made.known_new, stacks=made.stacks_new)


def solution(mesh):
    return jax.shard_map(
        on_device,
        mesh=mesh,
        in_specs=(
            P(ALONG, ACROSS, CHAN, None),
            P(ALONG, ACROSS, CHAN),
            P(CHAN),
            P(CHAN),
            P(ALONG, ACROSS),
            P(),
        ),
        out_specs=(
            P(ALONG, ACROSS, None),
            P(ALONG, ACROSS, None),
            P(ALONG, ACROSS, None),
        ),
        check_vma=False,
    )
```

```python
import jax
import jax.numpy as jnp
from jax import lax
from jax.experimental import pallas as pl
from jax.experimental.pallas import tpu as pltpu
from jax.sharding import PartitionSpec as P

BLOCKS = (2, 3, 5)
ALONG, ACROSS, CHAN = "along", "across", "chan"
S = 384
F32 = jnp.float32
VEC = (4, 8, S)
WIDE, BACK = (12, 2, 8, S), (8, 2, 8, S)


def params():
    return pltpu.CompilerParams(vmem_limit_bytes=16 * 1024 * 1024)


class Refs(dict):
    __getattr__ = dict.__getitem__


def call(kernel, outs, ins, scratch=()):
    vmem = pl.BlockSpec(memory_space=pltpu.VMEM)
    args, in_tree = jax.tree.flatten([*ins.values()])
    shapes, out_tree = jax.tree.flatten([*outs.values()], is_leaf=lambda v: isinstance(v, tuple))
    n, m = len(args), len(args) + len(shapes)

    def body(*refs):
        named = zip([*ins, *outs], in_tree.unflatten(refs[:n]) + out_tree.unflatten(refs[n:m]))
        kernel(Refs(named), *refs[m:])

    result = pl.pallas_call(
        body,
        out_shape=[jax.ShapeDtypeStruct(s, F32) for s in shapes],
        in_specs=[vmem] * len(args),
        out_specs=[vmem] * len(shapes),
        scratch_shapes=[pltpu.VMEM(s, F32) for s in scratch],
        compiler_params=params(),
    )(*args)
    return Refs(zip(outs, out_tree.unflatten(result)))


def back_through(g_ref, at, t):
    return jnp.concatenate(
        [
            jnp.sum(g_ref[at, :, 128 * n : 128 * (n + 1)] * t, axis=0, keepdims=True)
            for n in range(3)
        ],
        axis=1,
    )


def project(jac, field, wcol, flag, out):
    def row(i, carry):
        x8 = field[i]
        sums = []
        for j in range(8):
            y = jnp.sum(jac[i * 8 + j] * x8[j : j + 1, :], axis=1, keepdims=True)
            sums.append(back_through(jac, i * 8 + j, y * wcol[...]))
        out[i] = jnp.concatenate(sums, axis=0) * flag[i]
        return carry

    lax.fori_loop(0, 4, row, 0)


def column(row, size):
    lane = lax.broadcasted_iota(jnp.int32, (size, size), 1)
    sub = lax.broadcasted_iota(jnp.int32, (size, size), 0)
    return jnp.sum(jnp.where(lane == sub, jnp.broadcast_to(row, (size, size)), 0.0), axis=1, keepdims=True)


def first_kernel(
    place, jac_hbm, dep_hbm, inv_hbm, use_hbm, clear_hbm, coef_hbm,
    jac, wcol, flag, ctl, coefs, share, dep, inv, use, clear, coef, sems,
):
    pairs = [(inv_hbm, inv), (use_hbm, use), (clear_hbm, clear), (coef_hbm, coef), (dep_hbm, dep)]
    pairs += [(jac_hbm.at[pl.ds(8 * i, 8)], jac.at[pl.ds(8 * i, 8)]) for i in range(4)]
    copies = [pltpu.make_async_copy(*pair, sems.at[n]) for n, pair in enumerate(pairs)]
    for copy in copies:
        copy.start()
    for n in range(3):
        ctl[n] = jnp.broadcast_to(place[n], (8, 128)).astype(F32)
    low = lax.broadcasted_iota(jnp.int32, (8, 128), 0) < 4
    right, left = (jnp.broadcast_to(place[n], (8, 128)) for n in (3, 4))
    ctl[3] = jnp.where(low, right, left).astype(F32)
    for copy in copies[:5]:
        copy.wait()
    wcol[...] = jnp.broadcast_to(column(inv[...] * use[...].astype(F32), 128), (128, 128))
    for i in range(4):
        flag[i] = jnp.broadcast_to(column(clear[i : i + 1, :].astype(F32), 8), (8, S))
    for n in range(25):
        coefs[n] = jnp.broadcast_to(coef[n : n + 1, :], (8, S))

    def row(i, carry):
        pltpu.make_async_copy(
            jac_hbm.at[pl.ds(8 * i, 8)], jac.at[pl.ds(8 * i, 8)], sems.at[5 + i]
        ).wait()
        d8 = dep[i]
        sums = []
        for j in range(8):
            t = column(d8[j : j + 1, :], 128) * wcol[...]
            sums.append(back_through(jac, i * 8 + j, t))
        share[i] = jnp.concatenate(sums, axis=0) * flag[i]
        return carry

    lax.fori_loop(0, 4, row, 0)


def fold(v):
    s = (v[0] + v[1]) + (v[2] + v[3])
    return (s[:, :128] + s[:, 128:256]) + s[:, 256:]


def put(ref, at, v):
    for n in range(3):
        ref[at + n] = v[:, 128 * n : 128 * (n + 1)]


def get(ref, at):
    return jnp.concatenate([ref[at + n] for n in range(3)], axis=1)


def sum_kernel(r):
    total = (r.own[...] + r.far[...]) + (r.near[...] + r.other[...])
    r.total[...] = total
    for h in range(2):
        put(r.to_right, 3 * h, jnp.concatenate([total[2 * h][4:], total[2 * h + 1][4:]], axis=0))
        put(r.to_left, 3 * h, jnp.concatenate([total[2 * h][:4], total[2 * h + 1][:4]], axis=0))
    if "grams" in r:
        count = r.grams.shape[0]
        for n in range(count):
            g = r.grams[n]
            if n == count - 1:
                g = g + fold(r.uq[...] * total)
            r.scal[n] = g
            r.to_right[6 + n] = g
            r.to_left[6 + n] = g


def join_kernel(r):
    keep = r.ctl[3][:, :1]
    left, right = r.from_left, r.from_right
    for i in range(4):
        put(r.ext, 3 * i, r.total[i])
        h, k = 3 * (i // 2), 4 * (i % 2)
        side = jnp.concatenate([get(right, h)[k : k + 4], get(left, h)[k : k + 4]], axis=0)
        put(r.ext, 12 + 3 * i, jnp.where(keep > 0.5, side, 0.0))
    if "scal" in r:
        for n in range(r.scal.shape[0]):
            s = (r.scal[n] + r.opposite[n]) + (left[6 + n] + right[6 + n])
            r.ext[24 + n] = s
            r.plane[n] = s


def part_kernel(r):
    for n in range(r.part.shape[0]):
        r.part[n] = (r.facing[24 + n] + r.beside[n]) + r.opposite[n]


def shifted(mid, side, d):
    if d == 0:
        return mid, side
    if d > 0:
        return (
            jnp.concatenate([mid[d:], side[:d]], axis=0),
            jnp.concatenate([side[d:], mid[:d]], axis=0),
        )
    d = -d
    return (
        jnp.concatenate([side[8 - d :], mid[: 8 - d]], axis=0),
        jnp.concatenate([mid[8 - d :], side[: 8 - d]], axis=0),
    )


def stencil(r, wide, back, kw, kkw):
    ctl, coef = r.ctl, r.coef
    odd, up_ok, down_ok = ctl[0][:, :1] > 0.5, ctl[1][:, :1] > 0.5, ctl[2][:, :1] > 0.5
    for i in range(4):
        for part in range(2):
            at = 12 * part + 3 * i
            a, b = get(r.first, at), get(r.second, at)
            wide[i, part] = jnp.where(up_ok, jnp.where(odd, a, b), 0.0)
            wide[4 + i, part] = get(r.ext, at)
            wide[8 + i, part] = jnp.where(down_ok, jnp.where(odd, b, a), 0.0)
    side_ok = ctl[3][:, :1] > 0.5

    def back_row(i, carry):
        mid_sum = side_sum = 0.0
        for b in range(5):
            m = s = 0.0
            for a in range(5):
                c = coef[5 * a + b]
                m = m + c * wide[i + 4 - a, 0]
                s = s + c * wide[i + 4 - a, 1]
            m, s = shifted(m, s, 2 - b)
            mid_sum, side_sum = mid_sum + m, side_sum + s
        back[i, 0] = mid_sum
        back[i, 1] = jnp.where(side_ok, side_sum, 0.0)
        return carry

    lax.fori_loop(0, 8, back_row, 0)
    for i in range(2):
        for part in range(2):
            back[i, part] = jnp.where(up_ok, back[i, part], 0.0)
            back[6 + i, part] = jnp.where(down_ok, back[6 + i, part], 0.0)
    for i in range(4):
        kw[i] = back[i + 2, 0]

    def row(i, carry):
        total = 0.0
        for b in range(5):
            m = s = 0.0
            for a in range(5):
                c = coef[5 * a + b]
                m = m + c * back[i + a, 0]
                s = s + c * back[i + a, 1] if b != 2 else s
            total = total + (shifted(m, s, b - 2)[0] if b != 2 else m)
        kkw[i] = total
        return carry

    if kkw is not None:
        lax.fori_loop(0, 4, row, 0)


def start_kernel(r, wide, back):
    stencil(r, wide, back, r.u0, r.uq0)
    project(r.jac, r.uq0, r.wcol, r.flag, r.share)


def gram_rows(s, count):
    rows = [("t", k) for k in range(s)]
    rows += [("m", i, j) for i in range(s) for j in range(i, s) if i < s - 1]
    rows += [("x", n, k) for n in range(count) for k in range(s)]
    rows += [("f", n) for n in range(count)] + [("uu",)]
    return rows


def inner_kernel(k, s, count):
    def body(r, wide, back, kw, kkw):
        stencil(r, wide, back, kw, kkw)
        if "steer" in r:
            a, b = r.steer[0][:1, :1], r.steer[1][:1, :1]
        for basis, image, vector, q in ((r.us, r.image, r.u, kw), (r.uqs, r.imageq, r.uq, kkw)):
            v = basis[k - 1][...] + q[...]
            image[...] = v
            if "steer" in r:
                v = v - a * basis[k - 1][...]
                if k > 1:
                    v = v - b * basis[k - 2][...]
            vector[...] = v
        project(r.jac, r.uq, r.wcol, r.flag, r.share)
        if k < s - 1:
            return
        us, hus = [*r.us, r.u], [*r.hus, r.image]
        tiles = []
        for row in gram_rows(s, count):
            if row[0] == "t":
                x, y = us[row[1]][...], us[0][...]
            elif row[0] == "m":
                x, y = hus[row[1]][...], us[row[2]][...]
            elif row[0] == "x":
                x, y = r.hps[row[1]], us[row[2]][...]
            elif row[0] == "f":
                x, y = r.ps[row[1]], us[0][...]
            else:
                x, y = us[1][...], us[1][...]
            tiles.append(jnp.sum(fold(x * y), axis=0, keepdims=True))
        while len(tiles) % 8:
            tiles.append(jnp.zeros((1, 128), F32))
        for n in range(len(tiles) // 8):
            r.grams[n] = jnp.concatenate(tiles[8 * n : 8 * n + 8], axis=0)
        last = us[s - 1][...]
        r.grams[len(tiles) // 8] = fold(last * last)

    return body


def solve(scal, known, s, count, first):
    rows = gram_rows(s, count)
    packed = [jnp.sum(tile, axis=1, keepdims=True) for tile in scal[:-1]]
    splat = lambda v: jnp.broadcast_to(v, (8, 128))
    val = {row: splat(packed[n // 8][n % 8 : n % 8 + 1, :]) for n, row in enumerate(rows)}
    w = {(i, j): val["m", i, j] for i in range(s) for j in range(i, s) if i < s - 1}
    w[s - 1, s - 1] = splat(jnp.sum(scal[-1], axis=(0, 1), keepdims=True))
    y = [val["t", k] for k in range(s)]
    a = (1.6 if first else 1.1) * val["m", 0, 0] / y[0]
    b = (2.0 if first else 0.6) * (val["uu",] - y[1] * y[1] / y[0]) / y[0]
    inverse = [1.0 / known[n] for n in range(count)]
    old = [[val["x", n, k] * inverse[n] for k in range(s)] for n in range(count)]
    for n in range(count):
        for i in range(s):
            y[i] = y[i] - old[n][i] * val["f", n]
            for j in range(i, s):
                w[i, j] = w[i, j] - old[n][i] * val["x", n, j]
    new = {}
    for k in range(s):
        for i in range(k + 1, s):
            new[i, k] = w[k, i] / w[k, k]
        for i in range(k + 1, s):
            y[i] = y[i] - new[i, k] * y[k]
            for j in range(i, s):
                w[i, j] = w[i, j] - new[i, k] * w[k, j]
    fixes = [val["f", n] * inverse[n] for n in range(count)]
    pivots = [w[k, k] for k in range(s)]
    steps = [y[k] / w[k, k] for k in range(s)]
    row = lambda v: jnp.concatenate([v] * 3, axis=1)
    old = [[row(v) for v in vs] for vs in old]
    new = {key: row(v) for key, v in new.items()}
    return old, new, pivots, [row(v) for v in steps], [row(v) for v in fixes], (a, b)


def block_kernel(s, count, keep, first, final):
    def body(r, wide, back, kw, kkw):
        stencil(r, wide, back, kw, None if final else kkw)
        at = 24
        scal = [
            (r.ext[at + n] + r.first[at + n]) + (r.part[n] + r.mate[n])
            for n in range(r.part.shape[0])
        ]
        known = [r.known[n] for n in range(count)]
        old, new, pivots, steps, fixes, steer = solve(scal, known, s, count, first)

        def directions(i, stack, vectors):
            lasts = [r.stacks[stack][n, i] for n in range(count)]
            made = []
            for k, v in enumerate(vectors):
                for n in range(count):
                    v = v - old[n][k] * lasts[n]
                for j in range(k):
                    v = v - new[k, j] * made[j]
                made.append(v)
            if not final:
                for n, v in enumerate((lasts + made)[-keep:]):
                    r.stacks_new[stack][n, i] = v
            moved = steps[0] * made[0]
            for k in range(1, s):
                moved = moved + steps[k] * made[k]
            for n in range(count):
                moved = moved + fixes[n] * lasts[n]
            return moved

        def row(i, carry):
            us, uqs, hus, huqs = ([v[i] for v in vs] for vs in (r.us, r.uqs, r.hus, r.huqs))
            moved = directions(i, 0, us)
            r.x_new[i] = moved if first else r.x[i] + moved
            moved = directions(i, 1, uqs)
            r.xq_new[i] = moved if first else r.xq[i] + moved
            r.r_new[i] = us[0] - directions(i, 2, hus + [us[s - 1] + kw[i]])
            if not final:
                r.q_new[i] = uqs[0] - directions(i, 3, huqs + [uqs[s - 1] + kkw[i]])
            return carry

        lax.fori_loop(0, 4, row, 0)
        if final:
            return
        for n, v in enumerate((known + pivots)[-keep:]):
            r.known_new[n] = v
        for n, v in enumerate(steer):
            r.steer_new[n] = v
        project(r.jac, r.q_new, r.wcol, r.flag, r.share)

    return body


def move(x, axis, target):
    return lax.ppermute(x, axis, [(i, target(i)) for i in range(lax.axis_size(axis))])


def shift(x, axis, k):
    n = lax.axis_size(axis)
    return move(x, axis, lambda i: (i + k) % n)


def on_device(jacobian, departures, inv_variance, channel_use, clear_flags, coefficients):
    along, across = lax.axis_size(ALONG), lax.axis_size(ACROSS)
    a, c = lax.axis_index(ALONG), lax.axis_index(ACROSS)
    place = jnp.stack([a % 2, a > 0, a < along - 1, c < across - 1, c > 0]).astype(jnp.int32)
    vmem = pl.BlockSpec(memory_space=pltpu.VMEM)
    shapes = ((32, 128, S), (128, 128), VEC, (4, 8, 128), (25, 8, S), VEC)
    here = [((4, 8, 128), F32), ((1, 128), F32), ((1, 128), jnp.int32), ((4, 8), jnp.int32), ((25, S), F32)]
    jac, wcol, flag, ctl, coef, share = pl.pallas_call(
        first_kernel,
        out_shape=[pltpu.VMEM(s, F32) for s in shapes],
        in_specs=[pl.BlockSpec(memory_space=pltpu.SMEM)] + [pl.BlockSpec(memory_space=pl.ANY)] * 6,
        out_specs=[vmem] * 6,
        scratch_shapes=[pltpu.VMEM(*v) for v in here] + [pltpu.SemaphoreType.DMA((9,))],
        compiler_params=pltpu.CompilerParams(vmem_limit_bytes=48 * 1024 * 1024),
    )(
        place,
        jacobian.reshape(32, 128, S),
        departures,
        inv_variance[None],
        channel_use[None],
        clear_flags,
        coefficients,
    )
    consts = dict(ctl=ctl, coef=coef)
    sweep = dict(jac=jac, wcol=wcol, flag=flag)

    def exchange(share, sums=None):
        ins = dict(
            own=share,
            near=shift(share, CHAN, 1),
            far=shift(share, CHAN, 2),
            other=shift(share, CHAN, -1),
        )
        g = sums["grams"].shape[0] if sums else 0
        tail = (g, 8, 128)
        edge = (6 + g, 8, 128)
        outs = dict(total=VEC, to_right=edge, to_left=edge)
        if sums:
            ins |= sums
            outs |= dict(scal=tail)
        summed = call(sum_kernel, outs, ins)
        ins = dict(
            total=summed.total,
            from_left=shift(summed.to_right, ACROSS, 1),
            from_right=shift(summed.to_left, ACROSS, -1),
            ctl=ctl,
        )
        outs = dict(ext=(24 + g, 8, 128))
        if sums:
            ins |= dict(scal=summed.scal, opposite=shift(summed.scal, ACROSS, 2))
            outs |= dict(plane=tail)
        joined = call(join_kernel, outs, ins)
        ext = joined.ext
        near = dict(
            ext=ext,
            first=move(ext, ALONG, lambda i: i ^ 1),
            second=move(ext, ALONG, lambda i: (i - 1 if i % 2 == 0 else i + 1) % along),
        )
        if sums:
            plane = joined.plane
            ins = dict(
                facing=near["second"],
                beside=move(plane, ALONG, lambda i: (i + 2 if i % 2 == 0 else i - 2) % along),
                opposite=shift(plane, ALONG, 4),
            )
            part = call(part_kernel, dict(part=tail), ins).part
            near |= dict(part=part, mate=move(part, ALONG, lambda i: i ^ 1))
        return near | consts

    work = [WIDE, BACK]
    more = [WIDE, BACK, VEC, VEC]
    made = call(start_kernel, dict(u0=VEC, uq0=VEC, share=VEC), exchange(share) | sweep, work)
    us, uqs, hus, huqs = [made.u0], [made.uq0], [], []
    share = made.share
    state = old = steer = {}
    count = 0
    for number, s in enumerate(BLOCKS):
        final = number == len(BLOCKS) - 1
        for k in range(1, s):
            outs = dict(image=VEC, imageq=VEC, u=VEC, uq=VEC, share=VEC)
            ins = exchange(share) | sweep | steer | dict(us=us, uqs=uqs)
            if k == s - 1:
                outs |= dict(grams=(-(-len(gram_rows(s, count)) // 8) + 1, 8, 128))
                ins |= dict(hus=hus)
                if count:
                    ins |= dict(ps=old["stacks"][0], hps=old["stacks"][2])
            made = call(inner_kernel(k, s, count), outs, ins, more)
            share = made.share
            us, uqs = us + [made.u], uqs + [made.uq]
            hus, huqs = hus + [made.image], huqs + [made.imageq]
        near = exchange(share, dict(grams=made.grams, uq=made.uq))
        keep = 0 if final else min(count + s, BLOCKS[number + 1])
        ins = near | state | old | dict(us=us, uqs=uqs, hus=hus, huqs=huqs)
        outs = dict(x_new=VEC, xq_new=VEC, r_new=VEC)
        if not final:
            ins |= sweep
            outs |= dict(q_new=VEC, share=VEC, known_new=(keep, 8, 128), steer_new=(2, 8, 128))
            outs |= dict(stacks_new=[(keep, *VEC)] * 4)
        made = call(block_kernel(s, count, keep, number == 0, final), outs, ins, more)
        if final:
            return made.x_new, made.xq_new, made.r_new
        count = keep
        state = dict(x=made.x_new, xq=made.xq_new)
        us, uqs, hus, huqs = [made.r_new], [made.q_new], [], []
        share = made.share
        steer = dict(steer=made.steer_new)
        old = dict(known=made.known_new, stacks=made.stacks_new)


def solution(mesh):
    return jax.shard_map(
        on_device,
        mesh=mesh,
        in_specs=(
            P(ALONG, ACROSS, CHAN, None),
            P(ALONG, ACROSS, CHAN),
            P(CHAN),
            P(CHAN),
            P(ALONG, ACROSS),
            P(),
        ),
        out_specs=(
            P(ALONG, ACROSS, None),
            P(ALONG, ACROSS, None),
            P(ALONG, ACROSS, None),
        ),
        check_vma=False,
    )
```
